1024 devices in a mesh: role: 2 (over y_lo), space: 64 (over z, core), freq: 8 (over y_hi, x).
Axes of the slice: x: 4, y: 4 (y_hi: 2, y_lo: 2; y = y_hi * 2 + y_lo), z: 32, core: 2. Of those that a mesh axis runs over, the one named last changes fastest.
Arguments:
- fields: float32 [2, 5, 16, 8192], P('role', None, 'freq', 'space'), may hold values from -6 to 6
- spectra: float32 [2, 128, 4, 16, 8192], P('role', 'freq', None, None, 'space'), may hold values from -6 to 6
- freq_index: int32 [128], P('freq'), may hold values from 1 to 63
- freq_weight: float32 [128], P('freq'), may hold values from 0.5 to 2
- material_ids: int32 [16, 8192], P('freq', 'space'), may hold values from 0 to 7
- material: float32 [3, 8], replicated, may hold values from 0.5 to 2
- source_cells: int32 [2, 16], P('role'), may hold values from 0 to 131071
- wavelets: float32 [2, 8, 16], P('role'), may hold values from -6 to 6
Outputs:
- fields_out: float32 [2, 5, 16, 8192], P('role', None, 'freq', 'space')
- spectra_out: float32 [2, 128, 4, 16, 8192], P('role', 'freq', None, None, 'space')
- gradient: float32 [16, 8192], P(('role', 'freq'), 'space')
The draws below stay inside these ranges and needn't reach their ends.
Inputs may be any that keep to these rules, and one draw needn't show every extreme that they name: `source_cells`: cells may repeat.
All inputs are finite; a program needn't handle non-finite values.
Results may differ from the reference program's by a relative error of at most 0.0033.
Values may be sent and summed in bfloat16 or wider, within the bound.
No kernel may reach another device: no remote copies, remote signals or barrier semaphores. Data moves between devices by JAX's collectives and lax.ppermute only.
A program may use at most 32 MiB of HBM per device.

```python
import math
import jax
import jax.numpy as jnp
from jax import lax

F = 128
STEPS = 8
PERIOD = 64
NMAT = 8
NSRC = 16
NX = 16
NZ = 8192


def touch_ends(array, stream_key, least, largest):
    longest = array.shape.index(max(array.shape))
    spots = []
    for shift in (0, 1):
        where = [jax.random.randint(jax.random.fold_in(stream_key, axis), (), 0, length) for axis, length in enumerate(array.shape)]
        where[longest] = (where[longest] + shift) % array.shape[longest]
        spots.append(tuple(where))
    return array.at[spots[0]].set(least).at[spots[1]].set(largest)


def levels(own_key, dims, cuts, low, high):
    def one(axis_at, parts):
        draws = jax.random.uniform(jax.random.fold_in(jax.random.fold_in(own_key, 6), axis_at), (parts,), jnp.float32, low / len(cuts), high / len(cuts))
        return jnp.repeat(jnp.exp(draws), dims[axis_at] // parts).reshape((-1,) + (1,) * (len(dims) - axis_at - 1))

    factor_of = one(*cuts[0])
    for cut in cuts[1:]:
        factor_of = factor_of * one(*cut)
    return factor_of


def scatter_about(stream_key, dims, scale, limit, cuts=(), kind=jnp.bfloat16):
    level = levels(stream_key, dims, cuts, -0.22, 0.18) if cuts else 1.0
    array = jax.random.normal(stream_key, dims, jnp.float32) * scale * level
    return jnp.minimum(jnp.maximum(array, -limit), limit).astype(kind)


def setup_inputs(seed: int = 0) -> dict:
    keys = jax.random.split(jax.random.key(seed), 9)
    fields = scatter_about(keys[0], (2, 5, NX, NZ), 1.0, 6.0, ((0, 2), (2, 8), (3, 64)), jnp.float32)
    spectra = scatter_about(keys[1], (2, F, 4, NX, NZ), 1.0, 6.0, ((0, 2), (1, 8), (4, 64)), jnp.float32)
    freq_index = touch_ends(jax.random.randint(keys[2], (F,), 1, PERIOD), jax.random.fold_in(keys[2], 1), 1, PERIOD - 1).astype(jnp.int32)
    freq_weight = jnp.clip(jnp.exp(math.log(2.0) - 1.3862944 * jax.random.uniform(keys[3], (F,), jnp.float32) ** levels(keys[3], (F,), ((0, 8),), -0.2, 0.2)), 0.5, 2.0)
    material_ids = touch_ends(jax.random.randint(keys[4], (NX, NZ), 0, NMAT), jax.random.fold_in(keys[4], 1), 0, NMAT - 1).astype(jnp.int32)
    material = jnp.clip(jnp.exp(jax.random.uniform(keys[5], (3, NMAT), jnp.float32, math.log(0.5), math.log(2.0))), 0.5, 2.0)
    source_cells = touch_ends(jax.random.randint(keys[6], (2, NSRC), 0, NX * NZ), jax.random.fold_in(keys[6], 1), 0, (NX * NZ) - 1).astype(jnp.int32)
    wavelets = scatter_about(keys[7], (2, STEPS, NSRC), 1.0, 6.0, ((0, 2),), jnp.float32)
    return {"fields": fields, "spectra": spectra, "freq_index": freq_index, "freq_weight": freq_weight, "material_ids": material_ids, "material": material, "source_cells": source_cells, "wavelets": wavelets}


COURANT = 0.18
TWO_PI = 6.283185307179586


def twiddle_table(freq_index):
    times = jnp.arange(STEPS, dtype=jnp.int32)
    turns = (freq_index[:, None] * times[None, :]) % PERIOD
    angle = turns.astype(jnp.float32) * (TWO_PI / PERIOD)
    table = jnp.stack([jnp.cos(angle), -jnp.sin(angle)], axis=1)
    return table.reshape(-1, STEPS).astype(jnp.bfloat16)


def velocity_update(velocity, padded, buoyancy):
    sigma_xx = padded[0, 1:-1, 1:-1]
    sigma_zz = padded[1, 1:-1, 1:-1]
    sigma_xz = padded[2, 1:-1, 1:-1]
    vel_x = velocity[0] + COURANT * buoyancy * ((padded[0, 2:, 1:-1] - sigma_xx) + (sigma_xz - padded[2, 1:-1, :-2]))
    vel_z = velocity[1] + COURANT * buoyancy * ((sigma_xz - padded[2, :-2, 1:-1]) + (padded[1, 1:-1, 2:] - sigma_zz))
    return jnp.stack([vel_x, vel_z])


def stress_update(stress, padded, lame_first, lame_second, inject):
    vel_x = padded[0, 1:-1, 1:-1]
    vel_z = padded[1, 1:-1, 1:-1]
    strain_x = vel_x - padded[0, :-2, 1:-1]
    strain_z = vel_z - padded[1, 1:-1, :-2]
    stiff = lame_first + 2.0 * lame_second
    sigma_xx = stress[0] + COURANT * (stiff * strain_x + lame_first * strain_z) + inject
    sigma_zz = stress[1] + COURANT * (lame_first * strain_x + stiff * strain_z) + inject
    sigma_xz = stress[2] + COURANT * lame_second * ((padded[0, 1:-1, 2:] - vel_x) + (padded[1, 2:, 1:-1] - vel_z))
    return jnp.stack([sigma_xx, sigma_zz, sigma_xz])


def reference(fields, spectra, freq_index, freq_weight, material_ids, material, source_cells, wavelets):
    props = material[:, material_ids]
    buoyancy, lame_first, lame_second = props[0], props[1], props[2]
    table = twiddle_table(freq_index)
    widths = ((0, 0), (1, 1), (1, 1))
    new_fields = []
    new_spectra = []
    for which in range(2):
        velocity = fields[which, :2]
        stress = fields[which, 2:]
        snaps = []
        for tick in range(STEPS):
            velocity = velocity_update(velocity, jnp.pad(stress, widths), buoyancy)
            flat = jnp.zeros((NX * NZ,), jnp.float32).at[source_cells[which]].add(wavelets[which, tick])
            stress = stress_update(stress, jnp.pad(velocity, widths), lame_first, lame_second, flat.reshape(NX, NZ))
            snaps.append(velocity.astype(jnp.bfloat16))
        stacked = jnp.stack(snaps).reshape(STEPS, -1)
        spectral = jnp.dot(table, stacked, preferred_element_type=jnp.float32).reshape(F, 4, NX, NZ)
        new_spectra.append(spectra[which] + spectral)
        new_fields.append(jnp.concatenate([velocity, stress], axis=0))
    forward, adjoint = new_spectra[0], new_spectra[1]

    def accumulate(index, total):
        return total + freq_weight[index] * jnp.sum(forward[index] * adjoint[index], axis=0)

    gradient = lax.fori_loop(0, F, accumulate, jnp.zeros((NX, NZ), jnp.float32)) / F
    return jnp.stack(new_fields), jnp.stack(new_spectra), gradient
```

```python
import functools

import jax
import jax.numpy as jnp
from jax import lax
from jax.experimental import pallas as pl
from jax.experimental.pallas import tpu as pltpu
from jax.sharding import PartitionSpec as P

F = 128
STEPS = 8
PERIOD = 64
NMAT = 8
NFIELD = 5
NPROP = 3
COURANT = 0.18
TWO_PI = 6.283185307179586
LANES = 128
HALO = STEPS
ROW_PROPS = 10
ROW_CELLS = 16
ROW_INDEX = 17
ROW_WEIGHT = 18
ROW_WAVELET = 19
MSG_ROWS = 24
VMEM = pltpu.VMEM


def whole(space=VMEM):
    return pl.BlockSpec(memory_space=space)


def cost(flops, read):
    return pl.CostEstimate(flops=flops, bytes_accessed=read, transcendentals=0)


def lane_ids(shape):
    return lax.broadcasted_iota(jnp.int32, shape, len(shape) - 1)


def pack_fields(fields, ids, material, cells, index, weight, wavelets, message, tile, wide):
    tile[...] = jnp.zeros_like(tile)
    wide[...] = jnp.zeros_like(wide)
    for field in range(NFIELD):
        tile[2 * field : 2 * field + 2, :] = fields[field]
    which = ids[...]
    for prop in range(NPROP):
        value = jnp.zeros(which.shape, jnp.float32)
        for block in range(NMAT):
            value = jnp.where(which == block, material[prop, block], value)
        row = ROW_PROPS + 2 * prop
        tile[row : row + 2, :] = COURANT * value
    count = cells.shape[1]
    tile[ROW_CELLS : ROW_CELLS + 1, :count] = cells[...].astype(jnp.float32)
    tile[ROW_INDEX : ROW_INDEX + 1, : index.shape[1]] = index[...].astype(jnp.float32)
    tile[ROW_WEIGHT : ROW_WEIGHT + 1, : weight.shape[1]] = weight[...]
    wide[:, :count] = wavelets[...]
    spread = pltpu.roll(wide[...], 0, 1, stride=count, stride_axis=0)
    tile[ROW_WAVELET : ROW_WAVELET + 1, :] = jnp.sum(spread, axis=0, keepdims=True)
    value = tile[...]
    for target in range(message.shape[0]):
        message[target] = value


def pack_spectra(rows_all, parts, freqs, spectra, message):
    for row in range(rows_all):
        for part in range(parts):
            picked = spectra[pl.ds(part * rows_all + row, freqs, stride=parts * rows_all), :]
            message[row, part * freqs : (part + 1) * freqs, :] = picked.astype(jnp.bfloat16)


def unpack_fields(groups, received, center, edges):
    rows_all = 2 * groups
    lanes = lane_ids((rows_all, LANES))
    left = jnp.zeros((rows_all, LANES), jnp.float32)
    right = jnp.zeros((rows_all, LANES), jnp.float32)
    channels = [(role, 2 * field) for role in range(2) for field in range(NFIELD)]
    channels += [(0, ROW_PROPS + 2 * prop) for prop in range(NPROP)]
    for slot, (role, first) in enumerate(channels):
        for k in range(2):
            start = role * groups * MSG_ROWS + first + k
            center[pl.ds(slot * rows_all + k, groups, stride=2), :] = received[
                pl.ds(start, groups, stride=MSG_ROWS), :
            ]
        value = center[slot * rows_all : (slot + 1) * rows_all, :]
        low = jnp.where(lanes < HALO, value, 0.0)
        high = jnp.where(lanes >= LANES - HALO, value, 0.0)
        left = left + pltpu.roll(low, HALO * slot, 1)
        right = right + pltpu.roll(high, (HALO * slot + HALO) % LANES, 1)
    edges[0] = left
    edges[1] = right


def prepare(groups, freqs, count, width_all, received, inject, table, weights):
    rows_all = 2 * groups
    first_column = lax.axis_index("space") * LANES
    def joined(row):
        value = received[pl.ds(row, groups, stride=MSG_ROWS), :]
        spread = pltpu.roll(value, 0, 1, stride=freqs, stride_axis=0)
        return jnp.sum(spread, axis=0, keepdims=True)

    weights[...] = joined(ROW_WEIGHT)
    index = joined(ROW_INDEX).astype(jnp.int32)
    times = lax.broadcasted_iota(jnp.int32, (STEPS, LANES), 0)
    turns = lax.bitwise_and(index * times, PERIOD - 1)
    angle = turns.astype(jnp.float32) * (TWO_PI / PERIOD)
    table[:STEPS, :] = jnp.cos(angle).astype(jnp.bfloat16).astype(jnp.float32)
    table[STEPS:, :] = (-jnp.sin(angle)).astype(jnp.bfloat16).astype(jnp.float32)
    window = lax.broadcasted_iota(jnp.int32, (2 * LANES, LANES), 0)
    window = jnp.where(window < LANES + LANES // 2, window, window - 2 * LANES)
    row_ids = lax.broadcasted_iota(jnp.int32, (rows_all, LANES), 0)
    valid = lane_ids((rows_all, LANES)) < count
    for role in range(2):
        base = role * groups * MSG_ROWS
        cells = received[base + ROW_CELLS : base + ROW_CELLS + 1, :].astype(jnp.int32)
        cell_row = cells // width_all
        cell_column = cells - cell_row * width_all - first_column
        hit_column = jnp.where(window == cell_column, 1.0, 0.0)
        hit_row = jnp.logical_and(row_ids == cell_row, valid)
        amounts = received[base + ROW_WAVELET : base + ROW_WAVELET + 1, :]
        terms = []
        for tick in range(STEPS):
            shift = (LANES - tick * count) % LANES
            amount = pltpu.roll(jnp.broadcast_to(amounts, (rows_all, LANES)), shift, 1)
            terms.append(jnp.where(hit_row, amount, 0.0))
        left = jnp.concatenate(terms, axis=0)
        inject[role] = lax.dot_general(
            left,
            hit_column,
            (((1,), (1,)), ((), ())),
            precision=lax.Precision.HIGHEST,
            preferred_element_type=jnp.float32,
        )


def step_kernel(
    groups,
    freqs,
    center,
    halo_low,
    halo_high,
    inject,
    kron,
    spectra,
    fields_out,
    row_snaps,
    spectra_out,
    snaps,
    finals,
    held,
    read_sem,
    write_sem,
):
    rows_all = 2 * groups
    fetch = pltpu.make_async_copy(spectra, held, read_sem)
    fetch.start()
    own_role = lax.axis_index("role")
    own_group = lax.axis_index("freq")
    lanes = lane_ids((rows_all, LANES))
    row_ids = lax.broadcasted_iota(jnp.int32, (rows_all, 2 * LANES), 0)
    from_high = halo_high[...]
    from_low = halo_low[...]

    def extended(slot):
        middle = center[slot * rows_all : (slot + 1) * rows_all, :]
        after = pltpu.roll(from_high, (LANES - HALO * slot) % LANES, 1)
        before = pltpu.roll(from_low, (2 * LANES - HALO - HALO * slot) % LANES, 1)
        side = jnp.where(lanes < HALO, after, jnp.where(lanes >= LANES - HALO, before, 0.0))
        return jnp.concatenate([middle, side], axis=1)

    def up(value):
        return jnp.where(row_ids < rows_all - 1, pltpu.roll(value, rows_all - 1, 0), 0.0)

    def down(value):
        return jnp.where(row_ids > 0, pltpu.roll(value, 1, 0), 0.0)

    def after(value):
        return pltpu.roll(value, 2 * LANES - 1, 1)

    def before(value):
        return pltpu.roll(value, 1, 1)

    buoyancy, lame_first, lame_second = (extended(2 * NFIELD + prop) for prop in range(NPROP))
    stiff = lame_first + 2.0 * lame_second
    for role in range(2):
        vel_x, vel_z, sig_xx, sig_zz, sig_xz = (
            extended(role * NFIELD + field) for field in range(NFIELD)
        )
        for tick in range(STEPS):
            vel_x = vel_x + buoyancy * ((up(sig_xx) - sig_xx) + (sig_xz - before(sig_xz)))
            vel_z = vel_z + buoyancy * ((sig_xz - down(sig_xz)) + (after(sig_zz) - sig_zz))
            source = inject[role, tick * rows_all : (tick + 1) * rows_all, :]
            strain_x = vel_x - down(vel_x)
            strain_z = vel_z - before(vel_z)
            sig_xx = sig_xx + (stiff * strain_x + lame_first * strain_z) + source
            sig_zz = sig_zz + (lame_first * strain_x + stiff * strain_z) + source
            sig_xz = sig_xz + lame_second * ((after(vel_x) - vel_x) + (up(vel_z) - vel_z))
            for part, value in enumerate((vel_x, vel_z)):
                at = ((role * STEPS + tick) * 2 + part) * rows_all
                rounded = value[:, :LANES].astype(jnp.bfloat16).astype(jnp.float32)
                snaps[at : at + rows_all, :] = rounded
        for field, value in enumerate((vel_x, vel_z, sig_xx, sig_zz, sig_xz)):
            finals[role, field] = value[:, :LANES]
    for field in range(NFIELD):
        fields_out[field] = finals[own_role, field, pl.ds(2 * own_group, 2), :]
    own_row = own_role * groups + own_group
    for role in range(2):
        for part in range(2):
            start = (role * STEPS * 2 + part) * rows_all + own_row
            row_snaps[role, :, part * LANES : (part + 1) * LANES] = snaps[
                pl.ds(start, STEPS, stride=2 * rows_all), :
            ]
    base = own_role * (STEPS * 2 * rows_all)
    blocks = []
    for part in range(2):
        for half in range(rows_all // 8):
            pieces = [
                snaps[pl.ds(pl.multiple_of(base + (tick * 2 + part) * rows_all + half * 8, 8), 8), :]
                for tick in range(STEPS)
            ]
            blocks.append(jnp.concatenate(pieces, axis=0))
    right = jnp.concatenate(blocks, axis=1).astype(jnp.bfloat16)
    added = lax.dot_general(
        kron[...], right, (((1,), (0,)), ((), ())), preferred_element_type=jnp.float32
    )
    fetch.wait()
    per_freq = 4 * rows_all
    copies = []
    chunk = freqs // 4
    for freq in range(freqs):
        for phase in range(2):
            for part in range(2):
                for half in range(rows_all // 8):
                    at = freq * per_freq + (phase * 2 + part) * rows_all + half * 8
                    row = (freq * 2 + phase) * 8
                    column = (part * (rows_all // 8) + half) * LANES
                    held[at : at + 8, :] = (
                        held[at : at + 8, :] + added[row : row + 8, column : column + LANES]
                    )
        if (freq + 1) % chunk == 0:
            first = (freq + 1 - chunk) * per_freq
            span = pl.ds(first, chunk * per_freq)
            copy = pltpu.make_async_copy(
                held.at[span], spectra_out.at[span], write_sem.at[freq // chunk]
            )
            copy.start()
            copies.append(copy)
    for copy in copies:
        copy.wait()


def correlate(groups, freqs, received, row_snaps, table, weights, gradient):
    turned = table[...].astype(jnp.bfloat16)
    added = []
    for role in range(2):
        right = row_snaps[role].astype(jnp.bfloat16)
        phases = []
        for phase in range(2):
            phases.append(
                lax.dot_general(
                    turned[phase * STEPS : (phase + 1) * STEPS, :],
                    right,
                    (((0,), (0,)), ((), ())),
                    preferred_element_type=jnp.float32,
                )
            )
        added.append(phases)
    total = None
    for part in range(4):
        sides = []
        for role in range(2):
            pieces = [
                received[role * groups + group, part * freqs : (part + 1) * freqs, :]
                for group in range(groups)
            ]
            column = (part % 2) * LANES
            own = added[role][part // 2][:, column : column + LANES]
            sides.append(jnp.concatenate(pieces, axis=0).astype(jnp.float32) + own)
        product = sides[0] * sides[1]
        total = product if total is None else total + product
    gradient[...] = (
        lax.dot_general(
            weights[...],
            total,
            (((1,), (0,)), ((), ())),
            precision=lax.Precision.HIGHEST,
            preferred_element_type=jnp.float32,
        )
        * (1.0 / F)
    )


def phase_table(freq_index):
    freqs = freq_index.shape[0]
    shape = (freqs * 2 * 8, STEPS * 8)
    down = lax.broadcasted_iota(jnp.int32, shape, 0)
    across = lax.broadcasted_iota(jnp.int32, shape, 1)
    index = jnp.repeat(freq_index, 16)[:, None]
    turns = index * (across // 8) % PERIOD
    angle = turns.astype(jnp.float32) * (TWO_PI / PERIOD)
    value = jnp.where((down // 8) % 2 == 0, jnp.cos(angle), -jnp.sin(angle))
    return jnp.where(down % 8 == across % 8, value, 0.0).astype(jnp.bfloat16)


def f32(*shape):
    return jax.ShapeDtypeStruct(shape, jnp.float32)


def local(fields, spectra, freq_index, freq_weight, material_ids, material, source_cells, wavelets):
    groups = lax.axis_size("freq")
    members = 2 * groups
    freqs = freq_index.shape[0]
    rows_all = 2 * groups
    count = source_cells.shape[1]
    width_all = LANES * lax.axis_size("space")
    group_axes = ("role", "freq")
    flat = spectra.reshape(freqs * 4 * rows_all, LANES)

    message = pl.pallas_call(
        pack_fields,
        out_shape=f32(members, MSG_ROWS, LANES),
        in_specs=[whole(), whole(), whole(pltpu.SMEM), whole(), whole(), whole(), whole()],
        out_specs=whole(),
        scratch_shapes=[VMEM((MSG_ROWS, LANES), jnp.float32), VMEM((STEPS, LANES), jnp.float32)],
        cost_estimate=cost(100_000, 200_000),
        name="pack_fields",
    )(
        fields[0],
        material_ids,
        material,
        source_cells,
        freq_index[None],
        freq_weight[None],
        wavelets[0],
    )
    gathered = lax.all_to_all(message, group_axes, 0, 0, tiled=True)
    gathered = gathered.reshape(members * MSG_ROWS, LANES)

    row_message = pl.pallas_call(
        functools.partial(pack_spectra, rows_all, 4, freqs),
        out_shape=jax.ShapeDtypeStruct((rows_all, 4 * freqs, LANES), jnp.bfloat16),
        in_specs=[whole()],
        out_specs=whole(),
        cost_estimate=cost(2_000_000, 800_000),
        name="pack_spectra",
    )(flat)
    row_spectra = lax.all_to_all(row_message, group_axes, 0, 0, tiled=True)

    center, edges = pl.pallas_call(
        functools.partial(unpack_fields, groups),
        out_shape=[f32((2 * NFIELD + NPROP) * rows_all, LANES), f32(2, rows_all, LANES)],
        in_specs=[whole()],
        out_specs=[whole(), whole()],
        cost_estimate=cost(100_000, 300_000),
        name="unpack_fields",
    )(gathered)
    size = lax.axis_size("space")
    forward = [(i, i + 1) for i in range(size - 1)]
    backward = [(i + 1, i) for i in range(size - 1)]
    halo_low = lax.ppermute(edges[1], "space", forward)
    halo_high = lax.ppermute(edges[0], "space", backward)

    inject, table, weights = pl.pallas_call(
        functools.partial(prepare, groups, freqs, count, width_all),
        out_shape=[
            f32(2, STEPS * rows_all, 2 * LANES),
            f32(2 * STEPS, LANES),
            f32(1, LANES),
        ],
        in_specs=[whole()],
        out_specs=[whole()] * 3,
        cost_estimate=cost(2_000_000, 600_000),
        name="prepare",
    )(gathered)

    fields_out, row_snaps, spectra_out = pl.pallas_call(
        functools.partial(step_kernel, groups, freqs),
        out_shape=[
            f32(NFIELD, 2, LANES),
            f32(2, STEPS, 2 * LANES),
            f32(freqs * 4 * rows_all, LANES),
        ],
        in_specs=[whole()] * 5 + [whole(pl.ANY)],
        out_specs=[whole(), whole(), whole(pl.ANY)],
        scratch_shapes=[
            VMEM((2 * STEPS * 2 * rows_all, LANES), jnp.float32),
            VMEM((2, NFIELD, rows_all, LANES), jnp.float32),
            VMEM((freqs * 4 * rows_all, LANES), jnp.float32),
            pltpu.SemaphoreType.DMA,
            pltpu.SemaphoreType.DMA((4,)),
        ],
        cost_estimate=cost(20_000_000, 2_000_000),
        name="steps",
    )(center, halo_low, halo_high, inject, phase_table(freq_index), flat)

    gradient = pl.pallas_call(
        functools.partial(correlate, groups, freqs),
        out_shape=f32(1, LANES),
        in_specs=[whole()] * 4,
        out_specs=whole(),
        cost_estimate=cost(2_000_000, 600_000),
        name="correlate",
    )(row_spectra, row_snaps, table, weights)
    return fields_out[None], spectra_out.reshape(spectra.shape), gradient


def solution(mesh):
    return jax.shard_map(
        local,
        mesh=mesh,
        in_specs=(
            P("role", None, "freq", "space"),
            P("role", "freq", None, None, "space"),
            P("freq"),
            P("freq"),
            P("freq", "space"),
            P(),
            P("role", None),
            P("role", None, None),
        ),
        out_specs=(
            P("role", None, "freq", "space"),
            P("role", "freq", None, None, "space"),
            P(("role", "freq"), "space"),
        ),
        check_vma=False,
    )
```

```python
import functools

import jax
import jax.numpy as jnp
from jax import lax
from jax.experimental import pallas as pl
from jax.experimental.pallas import tpu as pltpu
from jax.sharding import PartitionSpec as P


F = 128
STEPS = 8
PERIOD = 64
NMAT = 8
NFIELD = 5
NPROP = 3
COURANT = 0.18
TWO_PI = 6.283185307179586
LANES = 128
HALO = STEPS
PARTS = 4
CHANNELS = NFIELD + NPROP
ROW_HALO = 2 * CHANNELS
ROW_CELL_ROW = 18
ROW_CELL_COLUMN = 19
ROW_INDEX = 20
ROW_WEIGHT = 21
ROW_WAVELET = 22
MSG_ROWS = 24
VMEM = pltpu.VMEM


def whole(space=VMEM):
    return pl.BlockSpec(memory_space=space)


def cost(flops, read):
    return pl.CostEstimate(flops=flops, bytes_accessed=read, transcendentals=0)


def params(kib):
    return pltpu.CompilerParams(vmem_limit_bytes=kib * 1024)


def lane_ids(shape):
    return lax.broadcasted_iota(jnp.int32, shape, len(shape) - 1)


def is_even():
    return lax.rem(lax.axis_index("space"), 2) == 0


def pack_block(
    width_all,
    fields_in,
    ids_in,
    material_in,
    cells_in,
    index_in,
    weight_in,
    wavelets_in,
    spectra_in,
    block,
    edge_chip,
    edge_link,
    spectra,
    fields,
    ids,
    material,
    cells,
    index,
    weight,
    wavelets,
    wide,
    sems,
):
    sources = (fields_in, ids_in, material_in, cells_in, index_in, weight_in, wavelets_in, spectra_in)
    targets = (fields, ids, material, cells, index, weight, wavelets, spectra)
    copies = [
        pltpu.make_async_copy(source, target, sems.at[slot])
        for slot, (source, target) in enumerate(zip(sources, targets))
    ]
    for copy in copies:
        copy.start()
    block[...] = jnp.zeros_like(block)
    wide[...] = jnp.zeros_like(wide)
    for copy in copies[:-1]:
        copy.wait()
    for field in range(NFIELD):
        block[2 * field : 2 * field + 2, :] = fields[field]
    which = ids[...]
    for prop in range(NPROP):
        value = jnp.zeros(which.shape, jnp.float32)
        for kind in range(NMAT):
            value = jnp.where(which == kind, material[prop, kind], value)
        row = 2 * (NFIELD + prop)
        block[row : row + 2, :] = COURANT * value
    count = cells.shape[1]
    cell_row = lax.div(cells[...], width_all)
    block[ROW_CELL_ROW : ROW_CELL_ROW + 1, :count] = cell_row.astype(jnp.float32)
    cell_column = cells[...] - cell_row * width_all
    block[ROW_CELL_COLUMN : ROW_CELL_COLUMN + 1, :count] = cell_column.astype(jnp.float32)
    block[ROW_INDEX : ROW_INDEX + 1, : index.shape[1]] = index[...].astype(jnp.float32)
    block[ROW_WEIGHT : ROW_WEIGHT + 1, : weight.shape[1]] = weight[...]
    wide[:, :count] = wavelets[...]
    spread = pltpu.roll(wide[...], 0, 1, stride=count, stride_axis=0)
    block[ROW_WAVELET : ROW_WAVELET + 1, :] = jnp.sum(spread, axis=0, keepdims=True)
    lanes = lane_ids((2, LANES))
    low = jnp.zeros((2, LANES), jnp.float32)
    high = jnp.zeros((2, LANES), jnp.float32)
    for slot in range(CHANNELS):
        value = block[2 * slot : 2 * slot + 2, :]
        left = jnp.where(lanes < HALO, value, 0.0)
        right = jnp.where(lanes >= LANES - HALO, value, 0.0)
        low = low + pltpu.roll(left, HALO * slot, 1)
        high = high + pltpu.roll(right, (HALO * slot + HALO) % LANES, 1)
    even = is_even()
    edge_chip[...] = jnp.where(even, high, low)
    edge_link[...] = jnp.where(even, low, high)
    copies[-1].wait()


def pack_message(freqs, block, from_chip, from_link, spectra, message, built, sems):
    rows_all = message.shape[0]
    even = is_even()
    before = jnp.where(even, from_link[...], from_chip[...])
    after = jnp.where(even, from_chip[...], from_link[...])
    block[ROW_HALO : ROW_HALO + 2, :] = before + pltpu.roll(after, LANES // 2, 1)
    exact = block[...]
    high = exact.astype(jnp.bfloat16).astype(jnp.float32)
    both = jnp.concatenate([high, exact - high], axis=0).astype(jnp.bfloat16)
    copies = []
    for row in range(rows_all):
        built[row, : 2 * MSG_ROWS, :] = both
        for part in range(PARTS):
            picked = spectra[pl.ds(part * rows_all + row, freqs, stride=PARTS * rows_all), :]
            first = 2 * MSG_ROWS + part * freqs
            built[row, first : first + freqs, :] = picked.astype(jnp.bfloat16)
        if row % 4 == 3:
            span = pl.ds(row - 3, 4)
            copy = pltpu.make_async_copy(built.at[span], message.at[span], sems.at[row // 4])
            copy.start()
            copies.append(copy)
    for copy in copies:
        copy.wait()


def twiddle(freqs, index, kron):
    span = 8 * STEPS
    lanes = lax.broadcasted_iota(jnp.int32, (freqs, freqs), 1)
    rows = lax.broadcasted_iota(jnp.int32, (freqs, freqs), 0)
    diagonal = jnp.where(lanes == rows, index[...].astype(jnp.float32), 0.0)
    column = jnp.sum(diagonal, axis=1, keepdims=True).astype(jnp.int32)
    across = lax.bitwise_and(lane_ids((freqs, 2 * span)), span - 1)
    turns = lax.bitwise_and(column * lax.shift_right_logical(across, 3), PERIOD - 1)
    angle = turns.astype(jnp.float32) * (TWO_PI / PERIOD)
    upper = lane_ids((freqs, 2 * span)) >= span
    value = jnp.where(upper, -jnp.sin(angle), jnp.cos(angle))
    keep = lax.bitwise_and(lane_ids((8, span)), 7) == lax.broadcasted_iota(
        jnp.int32, (8, span), 0
    )
    for freq in range(freqs):
        pair = []
        for phase in range(2):
            one = value[freq : freq + 1, phase * span : (phase + 1) * span]
            pair.append(jnp.where(keep, jnp.broadcast_to(one, (8, span)), 0.0))
        kron[freq * 16 : (freq + 1) * 16, :] = jnp.concatenate(pair, axis=0).astype(jnp.bfloat16)


def unpack(groups, received, decoded, center, halos):
    rows_all = 2 * groups
    for source in range(2 * groups):
        both = received[source, : 2 * MSG_ROWS, :].astype(jnp.float32)
        decoded[source * MSG_ROWS : (source + 1) * MSG_ROWS, :] = (
            both[:MSG_ROWS, :] + both[MSG_ROWS:, :]
        )

    def gather(target, at, role, first):
        for k in range(2):
            start = role * groups * MSG_ROWS + first + k
            target[pl.ds(at + k, groups, stride=2), :] = decoded[
                pl.ds(start, groups, stride=MSG_ROWS), :
            ]

    for role in range(2):
        for field in range(NFIELD):
            gather(center, (role * NFIELD + field) * rows_all, role, 2 * field)
        gather(halos, role * rows_all, role, ROW_HALO)
    for prop in range(NPROP):
        gather(center, (2 * NFIELD + prop) * rows_all, 0, 2 * (NFIELD + prop))


def prepare(groups, freqs, count, decoded, inject, table, weights):
    rows_all = 2 * groups
    first_column = lax.axis_index("space") * LANES

    def joined(row):
        value = decoded[pl.ds(row, groups, stride=MSG_ROWS), :]
        spread = pltpu.roll(value, 0, 1, stride=freqs, stride_axis=0)
        return jnp.sum(spread, axis=0, keepdims=True)

    weights[...] = joined(ROW_WEIGHT)
    index = joined(ROW_INDEX).astype(jnp.int32)
    times = lax.broadcasted_iota(jnp.int32, (STEPS, LANES), 0)
    turns = lax.bitwise_and(index * times, PERIOD - 1)
    angle = turns.astype(jnp.float32) * (TWO_PI / PERIOD)
    table[:STEPS, :] = jnp.cos(angle)
    table[STEPS:, :] = -jnp.sin(angle)
    window = lax.broadcasted_iota(jnp.int32, (2 * LANES, LANES), 0)
    window = jnp.where(window < LANES + LANES // 2, window, window - 2 * LANES)
    row_ids = lax.broadcasted_iota(jnp.int32, (rows_all, LANES), 0)
    lanes = lane_ids((rows_all, LANES))
    row_lanes = lane_ids((1, LANES))

    def twice(row):
        value = jnp.where(row_lanes < count, row, 0.0)
        return value + pltpu.roll(value, count, 1)

    for role in range(2):
        base = role * groups * MSG_ROWS
        cell_row = twice(decoded[base + ROW_CELL_ROW : base + ROW_CELL_ROW + 1, :])
        cell_column = twice(decoded[base + ROW_CELL_COLUMN : base + ROW_CELL_COLUMN + 1, :])
        near = cell_column.astype(jnp.int32) - first_column
        hit_column = jnp.where(window == near, 1.0, 0.0).astype(jnp.bfloat16)
        hit_row = jnp.logical_and(row_ids == cell_row.astype(jnp.int32), lanes < 2 * count)
        exact = decoded[base + ROW_WAVELET : base + ROW_WAVELET + 1, :]
        high = exact.astype(jnp.bfloat16).astype(jnp.float32)
        low = exact - high
        terms = []
        for tick in range(STEPS):
            first = pltpu.roll(high, (LANES - tick * count) % LANES, 1)
            second = pltpu.roll(low, (LANES + count - tick * count) % LANES, 1)
            amount = jnp.where(row_lanes < count, first, second)
            terms.append(jnp.where(hit_row, jnp.broadcast_to(amount, (rows_all, LANES)), 0.0))
        left = jnp.concatenate(terms, axis=0).astype(jnp.bfloat16)
        inject[role] = lax.dot_general(
            left, hit_column, (((1,), (1,)), ((), ())), preferred_element_type=jnp.float32
        )


def step_fields(groups, center, halos, inject, snaps, finals):
    rows_all = 2 * groups
    lanes = lane_ids((rows_all, LANES))
    row_ids = lax.broadcasted_iota(jnp.int32, (rows_all, 2 * LANES), 0)

    def extended(at, role, slot):
        middle = center[at * rows_all : (at + 1) * rows_all, :]
        halo = halos[role * rows_all : (role + 1) * rows_all, :]
        after = pltpu.roll(halo, (LANES + LANES // 2 - HALO * slot) % LANES, 1)
        before = pltpu.roll(halo, (2 * LANES - HALO - HALO * slot) % LANES, 1)
        side = jnp.where(lanes < HALO, after, jnp.where(lanes >= LANES - HALO, before, 0.0))
        return jnp.concatenate([middle, side], axis=1)

    def up(value):
        return jnp.where(row_ids < rows_all - 1, pltpu.roll(value, rows_all - 1, 0), 0.0)

    def down(value):
        return jnp.where(row_ids > 0, pltpu.roll(value, 1, 0), 0.0)

    def after(value):
        return pltpu.roll(value, 2 * LANES - 1, 1)

    def before(value):
        return pltpu.roll(value, 1, 1)

    buoyancy, lame_first, lame_second = (
        extended(2 * NFIELD + prop, 0, NFIELD + prop) for prop in range(NPROP)
    )
    stiff = lame_first + 2.0 * lame_second
    for role in range(2):
        vel_x, vel_z, sig_xx, sig_zz, sig_xz = (
            extended(role * NFIELD + field, role, field) for field in range(NFIELD)
        )
        for tick in range(STEPS):
            vel_x = vel_x + buoyancy * ((up(sig_xx) - sig_xx) + (sig_xz - before(sig_xz)))
            vel_z = vel_z + buoyancy * ((sig_xz - down(sig_xz)) + (after(sig_zz) - sig_zz))
            source = inject[role, tick * rows_all : (tick + 1) * rows_all, :]
            strain_x = vel_x - down(vel_x)
            strain_z = vel_z - before(vel_z)
            sig_xx = sig_xx + (stiff * strain_x + lame_first * strain_z) + source
            sig_zz = sig_zz + (lame_first * strain_x + stiff * strain_z) + source
            sig_xz = sig_xz + lame_second * ((after(vel_x) - vel_x) + (up(vel_z) - vel_z))
            for part, value in enumerate((vel_x, vel_z)):
                at = ((role * STEPS + tick) * 2 + part) * rows_all
                rounded = value[:, :LANES].astype(jnp.bfloat16).astype(jnp.float32)
                snaps[at : at + rows_all, :] = rounded
        for field, value in enumerate((vel_x, vel_z, sig_xx, sig_zz, sig_xz)):
            finals[role, field] = value[:, :LANES]


def correlate(groups, freqs, received, row_snaps, table, weights, gradient):
    turned = table[...].astype(jnp.bfloat16)
    added = []
    for role in range(2):
        right = row_snaps[role].astype(jnp.bfloat16)
        phases = []
        for phase in range(2):
            phases.append(
                lax.dot_general(
                    turned[phase * STEPS : (phase + 1) * STEPS, :],
                    right,
                    (((0,), (0,)), ((), ())),
                    preferred_element_type=jnp.float32,
                )
            )
        added.append(phases)
    total = None
    for part in range(PARTS):
        sides = []
        first = 2 * MSG_ROWS + part * freqs
        for role in range(2):
            pieces = [
                received[role * groups + group, first : first + freqs, :]
                for group in range(groups)
            ]
            column = (part % 2) * LANES
            own = added[role][part // 2][:, column : column + LANES]
            sides.append(jnp.concatenate(pieces, axis=0).astype(jnp.float32) + own)
        product = sides[0] * sides[1]
        total = product if total is None else total + product
    gradient[...] = (
        lax.dot_general(
            weights[...],
            total,
            (((1,), (0,)), ((), ())),
            precision=lax.Precision.HIGHEST,
            preferred_element_type=jnp.float32,
        )
        * (1.0 / F)
    )


def finish(
    groups,
    freqs,
    count,
    received,
    kron,
    spectra,
    fields_out,
    spectra_out,
    gradient_out,
    decoded,
    center,
    halos,
    inject,
    table,
    weights,
    snaps,
    finals,
    row_snaps,
    own_fields,
    gradient,
    held,
    sems,
):
    rows_all = 2 * groups
    own_role = lax.axis_index("role")
    own_group = lax.axis_index("freq")
    unpack(groups, received, decoded, center, halos)
    prepare(groups, freqs, count, decoded, inject, table, weights)
    step_fields(groups, center, halos, inject, snaps, finals)
    for field in range(NFIELD):
        own_fields[field] = finals[own_role, field, pl.ds(2 * own_group, 2), :]
    copies = [pltpu.make_async_copy(own_fields, fields_out, sems.at[0])]
    copies[0].start()
    base = own_role * (STEPS * 2 * rows_all)
    blocks = []
    for part in range(2):
        for half in range(rows_all // 8):
            pieces = [
                snaps[pl.ds(pl.multiple_of(base + (tick * 2 + part) * rows_all + half * 8, 8), 8), :]
                for tick in range(STEPS)
            ]
            blocks.append(jnp.concatenate(pieces, axis=0))
    right = jnp.concatenate(blocks, axis=1).astype(jnp.bfloat16)
    per_freq = PARTS * rows_all
    chunk = freqs // 4
    for step in range(4):
        added = lax.dot_general(
            kron[step * chunk * 16 : (step + 1) * chunk * 16, :],
            right,
            (((1,), (0,)), ((), ())),
            preferred_element_type=jnp.float32,
        )
        for freq in range(chunk):
            for phase in range(2):
                for part in range(2):
                    for half in range(rows_all // 8):
                        at = (step * chunk + freq) * per_freq
                        at = at + (phase * 2 + part) * rows_all + half * 8
                        row = (freq * 2 + phase) * 8
                        column = (part * (rows_all // 8) + half) * LANES
                        held[at : at + 8, :] = (
                            spectra[at : at + 8, :]
                            + added[row : row + 8, column : column + LANES]
                        )
        span = pl.ds(step * chunk * per_freq, chunk * per_freq)
        copy = pltpu.make_async_copy(held.at[span], spectra_out.at[span], sems.at[1 + step])
        copy.start()
        copies.append(copy)
    own_row = own_role * groups + own_group
    for role in range(2):
        for part in range(2):
            start = (role * STEPS * 2 + part) * rows_all + own_row
            row_snaps[role, :, part * LANES : (part + 1) * LANES] = snaps[
                pl.ds(start, STEPS, stride=2 * rows_all), :
            ]
    correlate(groups, freqs, received, row_snaps, table, weights, gradient)
    copy = pltpu.make_async_copy(gradient, gradient_out, sems.at[5])
    copy.start()
    copies.append(copy)
    for copy in copies:
        copy.wait()


def f32(*shape):
    return jax.ShapeDtypeStruct(shape, jnp.float32)


def in_hbm(*arrays):
    return [pltpu.with_memory_space_constraint(array, pltpu.HBM) for array in arrays]


def swaps(size, first):
    pairs = [(i, i + 1) for i in range(first, size - 1, 2)]
    return pairs + [(b, a) for a, b in pairs]


def program(fields, spectra, freq_index, freq_weight, material_ids, material, source_cells, wavelets):
    groups = lax.axis_size("freq")
    members = 2 * groups
    freqs = freq_index.shape[0]
    rows_all = 2 * groups
    count = source_cells.shape[1]
    size = lax.axis_size("space")
    flat = spectra.reshape(freqs * PARTS * rows_all, LANES)
    message_rows = 2 * MSG_ROWS + PARTS * freqs

    block, edge_chip, edge_link, held = pl.pallas_call(
        functools.partial(pack_block, LANES * size),
        out_shape=[
            VMEM((MSG_ROWS, LANES), jnp.float32),
            VMEM((2, LANES), jnp.float32),
            VMEM((2, LANES), jnp.float32),
            VMEM(flat.shape, jnp.float32),
        ],
        in_specs=[whole(pl.ANY)] * 8,
        out_specs=[whole()] * 4,
        scratch_shapes=[
            VMEM((NFIELD, 2, LANES), jnp.float32),
            VMEM((2, LANES), jnp.int32),
            pltpu.SMEM(material.shape, jnp.float32),
            VMEM((1, count), jnp.int32),
            VMEM((1, freqs), jnp.int32),
            VMEM((1, freqs), jnp.float32),
            VMEM((STEPS, count), jnp.float32),
            VMEM((STEPS, LANES), jnp.float32),
            pltpu.SemaphoreType.DMA((8,)),
        ],
        cost_estimate=cost(100_000, 40_000),
        compiler_params=params(1024),
        name="pack_block",
    )(
        *in_hbm(
            fields[0],
            material_ids,
            material,
            source_cells,
            freq_index[None],
            freq_weight[None],
            wavelets[0],
            flat,
        )
    )
    from_link = lax.ppermute(edge_link, "space", swaps(size, 1))
    from_chip = lax.ppermute(edge_chip, "space", swaps(size, 0))

    message = pl.pallas_call(
        functools.partial(pack_message, freqs),
        out_shape=jax.ShapeDtypeStruct((members, message_rows, LANES), jnp.bfloat16),
        in_specs=[whole()] * 4,
        out_specs=whole(pl.ANY),
        scratch_shapes=[
            VMEM((members, message_rows, LANES), jnp.bfloat16),
            pltpu.SemaphoreType.DMA((members // 4,)),
        ],
        cost_estimate=cost(2_000_000, 1_000_000),
        compiler_params=params(1536),
        name="pack_message",
    )(block, from_chip, from_link, held)
    received = lax.all_to_all(message, ("role", "freq"), 0, 0, tiled=True)

    kron = pl.pallas_call(
        functools.partial(twiddle, freqs),
        out_shape=jax.ShapeDtypeStruct((freqs * 16, STEPS * 8), jnp.bfloat16),
        in_specs=[whole()],
        out_specs=whole(),
        cost_estimate=cost(100_000, 40_000),
        compiler_params=params(512),
        name="twiddle",
    )(freq_index[None])

    fields_out, spectra_out, gradient = pl.pallas_call(
        functools.partial(finish, groups, freqs, count),
        out_shape=[
            f32(NFIELD, 2, LANES),
            f32(freqs * PARTS * rows_all, LANES),
            f32(1, LANES),
        ],
        in_specs=[whole()] * 3,
        out_specs=[whole(pl.ANY)] * 3,
        scratch_shapes=[
            VMEM((members * MSG_ROWS, LANES), jnp.float32),
            VMEM(((2 * NFIELD + NPROP) * rows_all, LANES), jnp.float32),
            VMEM((2 * rows_all, LANES), jnp.float32),
            VMEM((2, STEPS * rows_all, 2 * LANES), jnp.float32),
            VMEM((2 * STEPS, LANES), jnp.float32),
            VMEM((1, LANES), jnp.float32),
            VMEM((2 * STEPS * 2 * rows_all, LANES), jnp.float32),
            VMEM((2, NFIELD, rows_all, LANES), jnp.float32),
            VMEM((2, STEPS, 2 * LANES), jnp.float32),
            VMEM((NFIELD, 2, LANES), jnp.float32),
            VMEM((1, LANES), jnp.float32),
            VMEM((freqs * PARTS * rows_all, LANES), jnp.float32),
            pltpu.SemaphoreType.DMA((6,)),
        ],
        cost_estimate=cost(20_000_000, 2_000_000),
        compiler_params=params(4096),
        name="finish",
    )(received, kron, held)
    return fields_out[None], spectra_out.reshape(spectra.shape), gradient


def solution(mesh):
    return jax.shard_map(
        program,
        mesh=mesh,
        in_specs=(
            P("role", None, "freq", "space"),
            P("role", "freq", None, None, "space"),
            P("freq"),
            P("freq"),
            P("freq", "space"),
            P(),
            P("role", None),
            P("role", None, None),
        ),
        out_specs=(
            P("role", None, "freq", "space"),
            P("role", "freq", None, None, "space"),
            P(("role", "freq"), "space"),
        ),
        check_vma=False,
    )
```

```python
import functools

import jax
import jax.numpy as jnp
from jax import lax
from jax.experimental import pallas as pl
from jax.experimental.pallas import tpu as pltpu
from jax.sharding import PartitionSpec as P


F = 128
STEPS = 8
PERIOD = 64
NMAT = 8
NFIELD = 5
NPROP = 3
COURANT = 0.18
TWO_PI = 6.283185307179586
LANES = 128
HALO = STEPS
PARTS = 4
CHANNELS = NFIELD + NPROP
ROW_HALO = 2 * CHANNELS
ROW_CELL_ROW = 18
ROW_CELL_COLUMN = 19
ROW_INDEX = 20
ROW_WEIGHT = 21
ROW_WAVELET = 22
MSG_ROWS = 24
VMEM = pltpu.VMEM


def whole(space=VMEM):
    return pl.BlockSpec(memory_space=space)


def cost(flops, read):
    return pl.CostEstimate(flops=flops, bytes_accessed=read, transcendentals=0)


def params(kib):
    return pltpu.CompilerParams(vmem_limit_bytes=kib * 1024)


def lane_ids(shape):
    return lax.broadcasted_iota(jnp.int32, shape, len(shape) - 1)


def is_even():
    return lax.rem(lax.axis_index("space"), 2) == 0


def pack_block(
    width_all,
    fields_in,
    ids_in,
    material_in,
    cells_in,
    index_in,
    weight_in,
    wavelets_in,
    spectra_in,
    block,
    edge_chip,
    edge_link,
    spectra,
    fields,
    ids,
    material,
    cells,
    index,
    weight,
    wavelets,
    wide,
    sems,
):
    sources = (fields_in, ids_in, material_in, cells_in, index_in, weight_in, wavelets_in, spectra_in)
    targets = (fields, ids, material, cells, index, weight, wavelets, spectra)
    copies = [
        pltpu.make_async_copy(source, target, sems.at[slot])
        for slot, (source, target) in enumerate(zip(sources, targets))
    ]
    for copy in copies:
        copy.start()
    block[...] = jnp.zeros_like(block)
    wide[...] = jnp.zeros_like(wide)
    for copy in copies[:-1]:
        copy.wait()
    for field in range(NFIELD):
        block[2 * field : 2 * field + 2, :] = fields[field]
    which = ids[...]
    for prop in range(NPROP):
        value = jnp.zeros(which.shape, jnp.float32)
        for kind in range(NMAT):
            value = jnp.where(which == kind, material[prop, kind], value)
        row = 2 * (NFIELD + prop)
        block[row : row + 2, :] = COURANT * value
    count = cells.shape[1]
    cell_row = lax.div(cells[...], width_all)
    block[ROW_CELL_ROW : ROW_CELL_ROW + 1, :count] = cell_row.astype(jnp.float32)
    cell_column = cells[...] - cell_row * width_all
    block[ROW_CELL_COLUMN : ROW_CELL_COLUMN + 1, :count] = cell_column.astype(jnp.float32)
    block[ROW_INDEX : ROW_INDEX + 1, : index.shape[1]] = index[...].astype(jnp.float32)
    block[ROW_WEIGHT : ROW_WEIGHT + 1, : weight.shape[1]] = weight[...]
    wide[:, :count] = wavelets[...]
    spread = pltpu.roll(wide[...], 0, 1, stride=count, stride_axis=0)
    block[ROW_WAVELET : ROW_WAVELET + 1, :] = jnp.sum(spread, axis=0, keepdims=True)
    lanes = lane_ids((2, LANES))
    low = jnp.zeros((2, LANES), jnp.float32)
    high = jnp.zeros((2, LANES), jnp.float32)
    for slot in range(CHANNELS):
        value = block[2 * slot : 2 * slot + 2, :]
        left = jnp.where(lanes < HALO, value, 0.0)
        right = jnp.where(lanes >= LANES - HALO, value, 0.0)
        low = low + pltpu.roll(left, HALO * slot, 1)
        high = high + pltpu.roll(right, (HALO * slot + HALO) % LANES, 1)
    even = is_even()
    edge_chip[...] = jnp.where(even, high, low)
    edge_link[...] = jnp.where(even, low, high)
    copies[-1].wait()


def pack_spectra(freqs, spectra, message):
    rows_all = message.shape[0]
    for row in range(rows_all):
        for part in range(PARTS):
            picked = spectra[pl.ds(part * rows_all + row, freqs, stride=PARTS * rows_all), :]
            message[row, part * freqs : (part + 1) * freqs, :] = picked.astype(jnp.bfloat16)


def pack_rows(block, from_chip, from_link, row_spectra, message, tile):
    even = is_even()
    before = jnp.where(even, from_link[...], from_chip[...])
    after = jnp.where(even, from_chip[...], from_link[...])
    tile[...] = block[...]
    tile[ROW_HALO : ROW_HALO + 2, :] = before + pltpu.roll(after, LANES // 2, 1)
    exact = tile[...]
    high = exact.astype(jnp.bfloat16).astype(jnp.float32)
    both = jnp.concatenate([high, exact - high], axis=0).astype(jnp.bfloat16)
    for row in range(message.shape[0]):
        message[row, : 2 * MSG_ROWS, :] = both
        message[row, 2 * MSG_ROWS :, :] = row_spectra[row]


def twiddle(freqs, block, kron):
    span = 8 * STEPS
    lanes = lax.broadcasted_iota(jnp.int32, (freqs, freqs), 1)
    rows = lax.broadcasted_iota(jnp.int32, (freqs, freqs), 0)
    index = block[ROW_INDEX : ROW_INDEX + 1, :freqs]
    diagonal = jnp.where(lanes == rows, index, 0.0)
    column = jnp.sum(diagonal, axis=1, keepdims=True).astype(jnp.int32)
    across = lax.bitwise_and(lane_ids((freqs, 2 * span)), span - 1)
    turns = lax.bitwise_and(column * lax.shift_right_logical(across, 3), PERIOD - 1)
    angle = turns.astype(jnp.float32) * (TWO_PI / PERIOD)
    upper = lane_ids((freqs, 2 * span)) >= span
    value = jnp.where(upper, -jnp.sin(angle), jnp.cos(angle))
    keep = lax.bitwise_and(lane_ids((8, span)), 7) == lax.broadcasted_iota(
        jnp.int32, (8, span), 0
    )
    for freq in range(freqs):
        pair = []
        for phase in range(2):
            one = value[freq : freq + 1, phase * span : (phase + 1) * span]
            pair.append(jnp.where(keep, jnp.broadcast_to(one, (8, span)), 0.0))
        kron[freq * 16 : (freq + 1) * 16, :] = jnp.concatenate(pair, axis=0).astype(jnp.bfloat16)


def unpack(groups, received, decoded, center, halos):
    rows_all = 2 * groups
    for source in range(2 * groups):
        both = received[source, : 2 * MSG_ROWS, :].astype(jnp.float32)
        decoded[source * MSG_ROWS : (source + 1) * MSG_ROWS, :] = (
            both[:MSG_ROWS, :] + both[MSG_ROWS:, :]
        )

    def gather(target, at, role, first):
        for k in range(2):
            start = role * groups * MSG_ROWS + first + k
            target[pl.ds(at + k, groups, stride=2), :] = decoded[
                pl.ds(start, groups, stride=MSG_ROWS), :
            ]

    for role in range(2):
        for field in range(NFIELD):
            gather(center, (role * NFIELD + field) * rows_all, role, 2 * field)
        gather(halos, role * rows_all, role, ROW_HALO)
    for prop in range(NPROP):
        gather(center, (2 * NFIELD + prop) * rows_all, 0, 2 * (NFIELD + prop))


def prepare(groups, freqs, count, decoded, inject, table, weights):
    rows_all = 2 * groups
    first_column = lax.axis_index("space") * LANES

    def joined(row):
        value = decoded[pl.ds(row, groups, stride=MSG_ROWS), :]
        spread = pltpu.roll(value, 0, 1, stride=freqs, stride_axis=0)
        return jnp.sum(spread, axis=0, keepdims=True)

    weights[...] = joined(ROW_WEIGHT)
    index = joined(ROW_INDEX).astype(jnp.int32)
    times = lax.broadcasted_iota(jnp.int32, (STEPS, LANES), 0)
    turns = lax.bitwise_and(index * times, PERIOD - 1)
    angle = turns.astype(jnp.float32) * (TWO_PI / PERIOD)
    table[:STEPS, :] = jnp.cos(angle)
    table[STEPS:, :] = -jnp.sin(angle)
    window = lax.broadcasted_iota(jnp.int32, (2 * LANES, LANES), 0)
    window = jnp.where(window < LANES + LANES // 2, window, window - 2 * LANES)
    row_ids = lax.broadcasted_iota(jnp.int32, (rows_all, LANES), 0)
    lanes = lane_ids((rows_all, LANES))
    row_lanes = lane_ids((1, LANES))

    def twice(row):
        value = jnp.where(row_lanes < count, row, 0.0)
        return value + pltpu.roll(value, count, 1)

    for role in range(2):
        base = role * groups * MSG_ROWS
        cell_row = twice(decoded[base + ROW_CELL_ROW : base + ROW_CELL_ROW + 1, :])
        cell_column = twice(decoded[base + ROW_CELL_COLUMN : base + ROW_CELL_COLUMN + 1, :])
        near = cell_column.astype(jnp.int32) - first_column
        hit_column = jnp.where(window == near, 1.0, 0.0).astype(jnp.bfloat16)
        hit_row = jnp.logical_and(row_ids == cell_row.astype(jnp.int32), lanes < 2 * count)
        exact = decoded[base + ROW_WAVELET : base + ROW_WAVELET + 1, :]
        high = exact.astype(jnp.bfloat16).astype(jnp.float32)
        low = exact - high
        terms = []
        for tick in range(STEPS):
            first = pltpu.roll(high, (LANES - tick * count) % LANES, 1)
            second = pltpu.roll(low, (LANES + count - tick * count) % LANES, 1)
            amount = jnp.where(row_lanes < count, first, second)
            terms.append(jnp.where(hit_row, jnp.broadcast_to(amount, (rows_all, LANES)), 0.0))
        left = jnp.concatenate(terms, axis=0).astype(jnp.bfloat16)
        inject[role] = lax.dot_general(
            left, hit_column, (((1,), (1,)), ((), ())), preferred_element_type=jnp.float32
        )


def step_fields(groups, center, halos, inject, snaps, finals):
    rows_all = 2 * groups
    lanes = lane_ids((rows_all, LANES))
    row_ids = lax.broadcasted_iota(jnp.int32, (rows_all, 2 * LANES), 0)

    def extended(at, role, slot):
        middle = center[at * rows_all : (at + 1) * rows_all, :]
        halo = halos[role * rows_all : (role + 1) * rows_all, :]
        after = pltpu.roll(halo, (LANES + LANES // 2 - HALO * slot) % LANES, 1)
        before = pltpu.roll(halo, (2 * LANES - HALO - HALO * slot) % LANES, 1)
        side = jnp.where(lanes < HALO, after, jnp.where(lanes >= LANES - HALO, before, 0.0))
        return jnp.concatenate([middle, side], axis=1)

    def up(value):
        return jnp.where(row_ids < rows_all - 1, pltpu.roll(value, rows_all - 1, 0), 0.0)

    def down(value):
        return jnp.where(row_ids > 0, pltpu.roll(value, 1, 0), 0.0)

    def after(value):
        return pltpu.roll(value, 2 * LANES - 1, 1)

    def before(value):
        return pltpu.roll(value, 1, 1)

    buoyancy, lame_first, lame_second = (
        extended(2 * NFIELD + prop, 0, NFIELD + prop) for prop in range(NPROP)
    )
    stiff = lame_first + 2.0 * lame_second
    for role in range(2):
        vel_x, vel_z, sig_xx, sig_zz, sig_xz = (
            extended(role * NFIELD + field, role, field) for field in range(NFIELD)
        )
        for tick in range(STEPS):
            vel_x = vel_x + buoyancy * ((up(sig_xx) - sig_xx) + (sig_xz - before(sig_xz)))
            vel_z = vel_z + buoyancy * ((sig_xz - down(sig_xz)) + (after(sig_zz) - sig_zz))
            source = inject[role, tick * rows_all : (tick + 1) * rows_all, :]
            strain_x = vel_x - down(vel_x)
            strain_z = vel_z - before(vel_z)
            sig_xx = sig_xx + (stiff * strain_x + lame_first * strain_z) + source
            sig_zz = sig_zz + (lame_first * strain_x + stiff * strain_z) + source
            sig_xz = sig_xz + lame_second * ((after(vel_x) - vel_x) + (up(vel_z) - vel_z))
            for part, value in enumerate((vel_x, vel_z)):
                at = ((role * STEPS + tick) * 2 + part) * rows_all
                rounded = value[:, :LANES].astype(jnp.bfloat16).astype(jnp.float32)
                snaps[at : at + rows_all, :] = rounded
        for field, value in enumerate((vel_x, vel_z, sig_xx, sig_zz, sig_xz)):
            finals[role, field] = value[:, :LANES]


def correlate(groups, freqs, received, row_snaps, table, weights, gradient):
    turned = table[...].astype(jnp.bfloat16)
    added = []
    for role in range(2):
        right = row_snaps[role].astype(jnp.bfloat16)
        phases = []
        for phase in range(2):
            phases.append(
                lax.dot_general(
                    turned[phase * STEPS : (phase + 1) * STEPS, :],
                    right,
                    (((0,), (0,)), ((), ())),
                    preferred_element_type=jnp.float32,
                )
            )
        added.append(phases)
    total = None
    for part in range(PARTS):
        sides = []
        first = 2 * MSG_ROWS + part * freqs
        for role in range(2):
            pieces = [
                received[role * groups + group, first : first + freqs, :]
                for group in range(groups)
            ]
            column = (part % 2) * LANES
            own = added[role][part // 2][:, column : column + LANES]
            sides.append(jnp.concatenate(pieces, axis=0).astype(jnp.float32) + own)
        product = sides[0] * sides[1]
        total = product if total is None else total + product
    gradient[...] = (
        lax.dot_general(
            weights[...],
            total,
            (((1,), (0,)), ((), ())),
            precision=lax.Precision.HIGHEST,
            preferred_element_type=jnp.float32,
        )
        * (1.0 / F)
    )


def finish(
    groups,
    freqs,
    count,
    received,
    kron,
    spectra,
    fields_out,
    spectra_out,
    gradient_out,
    decoded,
    center,
    halos,
    inject,
    table,
    weights,
    snaps,
    finals,
    row_snaps,
    own_fields,
    gradient,
    held,
    sems,
):
    rows_all = 2 * groups
    own_role = lax.axis_index("role")
    own_group = lax.axis_index("freq")
    unpack(groups, received, decoded, center, halos)
    prepare(groups, freqs, count, decoded, inject, table, weights)
    step_fields(groups, center, halos, inject, snaps, finals)
    for field in range(NFIELD):
        own_fields[field] = finals[own_role, field, pl.ds(2 * own_group, 2), :]
    copies = [pltpu.make_async_copy(own_fields, fields_out, sems.at[0])]
    copies[0].start()
    base = own_role * (STEPS * 2 * rows_all)
    blocks = []
    for part in range(2):
        for half in range(rows_all // 8):
            pieces = [
                snaps[pl.ds(pl.multiple_of(base + (tick * 2 + part) * rows_all + half * 8, 8), 8), :]
                for tick in range(STEPS)
            ]
            blocks.append(jnp.concatenate(pieces, axis=0))
    right = jnp.concatenate(blocks, axis=1).astype(jnp.bfloat16)
    per_freq = PARTS * rows_all
    chunk = freqs // 4
    for step in range(4):
        added = lax.dot_general(
            kron[step * chunk * 16 : (step + 1) * chunk * 16, :],
            right,
            (((1,), (0,)), ((), ())),
            preferred_element_type=jnp.float32,
        )
        for freq in range(chunk):
            for phase in range(2):
                for part in range(2):
                    for half in range(rows_all // 8):
                        at = (step * chunk + freq) * per_freq
                        at = at + (phase * 2 + part) * rows_all + half * 8
                        row = (freq * 2 + phase) * 8
                        column = (part * (rows_all // 8) + half) * LANES
                        held[at : at + 8, :] = (
                            spectra[at : at + 8, :]
                            + added[row : row + 8, column : column + LANES]
                        )
        span = pl.ds(step * chunk * per_freq, chunk * per_freq)
        copy = pltpu.make_async_copy(held.at[span], spectra_out.at[span], sems.at[1 + step])
        copy.start()
        copies.append(copy)
    own_row = own_role * groups + own_group
    for role in range(2):
        for part in range(2):
            start = (role * STEPS * 2 + part) * rows_all + own_row
            row_snaps[role, :, part * LANES : (part + 1) * LANES] = snaps[
                pl.ds(start, STEPS, stride=2 * rows_all), :
            ]
    correlate(groups, freqs, received, row_snaps, table, weights, gradient)
    copy = pltpu.make_async_copy(gradient, gradient_out, sems.at[5])
    copy.start()
    copies.append(copy)
    for copy in copies:
        copy.wait()


def f32(*shape):
    return jax.ShapeDtypeStruct(shape, jnp.float32)


def in_hbm(*arrays):
    return [pltpu.with_memory_space_constraint(array, pltpu.HBM) for array in arrays]


def swaps(size, first):
    pairs = [(i, i + 1) for i in range(first, size - 1, 2)]
    return pairs + [(b, a) for a, b in pairs]


def program(fields, spectra, freq_index, freq_weight, material_ids, material, source_cells, wavelets):
    groups = lax.axis_size("freq")
    members = 2 * groups
    freqs = freq_index.shape[0]
    rows_all = 2 * groups
    count = source_cells.shape[1]
    size = lax.axis_size("space")
    flat = spectra.reshape(freqs * PARTS * rows_all, LANES)
    message_rows = 2 * MSG_ROWS + PARTS * freqs

    block, edge_chip, edge_link, held = pl.pallas_call(
        functools.partial(pack_block, LANES * size),
        out_shape=[
            VMEM((MSG_ROWS, LANES), jnp.float32),
            VMEM((2, LANES), jnp.float32),
            VMEM((2, LANES), jnp.float32),
            VMEM(flat.shape, jnp.float32),
        ],
        in_specs=[whole(pl.ANY)] * 8,
        out_specs=[whole()] * 4,
        scratch_shapes=[
            VMEM((NFIELD, 2, LANES), jnp.float32),
            VMEM((2, LANES), jnp.int32),
            pltpu.SMEM(material.shape, jnp.float32),
            VMEM((1, count), jnp.int32),
            VMEM((1, freqs), jnp.int32),
            VMEM((1, freqs), jnp.float32),
            VMEM((STEPS, count), jnp.float32),
            VMEM((STEPS, LANES), jnp.float32),
            pltpu.SemaphoreType.DMA((8,)),
        ],
        cost_estimate=cost(100_000, 40_000),
        compiler_params=params(1024),
        name="pack_block",
    )(
        *in_hbm(
            fields[0],
            material_ids,
            material,
            source_cells,
            freq_index[None],
            freq_weight[None],
            wavelets[0],
            flat,
        )
    )
    from_link = lax.ppermute(edge_link, "space", swaps(size, 1))
    from_chip = lax.ppermute(edge_chip, "space", swaps(size, 0))

    kron = pl.pallas_call(
        functools.partial(twiddle, freqs),
        out_shape=jax.ShapeDtypeStruct((freqs * 16, STEPS * 8), jnp.bfloat16),
        in_specs=[whole()],
        out_specs=whole(),
        cost_estimate=cost(100_000, 40_000),
        compiler_params=params(512),
        name="twiddle",
    )(block)

    row_spectra = pl.pallas_call(
        functools.partial(pack_spectra, freqs),
        out_shape=VMEM((members, PARTS * freqs, LANES), jnp.bfloat16),
        in_specs=[whole()],
        out_specs=whole(),
        cost_estimate=cost(2_000_000, 1_000_000),
        compiler_params=params(1536),
        name="pack_spectra",
    )(held)
    message = pl.pallas_call(
        pack_rows,
        out_shape=VMEM((members, message_rows, LANES), jnp.bfloat16),
        in_specs=[whole()] * 4,
        out_specs=whole(),
        scratch_shapes=[VMEM((MSG_ROWS, LANES), jnp.float32)],
        cost_estimate=cost(100_000, 300_000),
        compiler_params=params(2048),
        name="pack_rows",
    )(block, from_chip, from_link, row_spectra)
    received = lax.all_to_all(message, ("role", "freq"), 0, 0, tiled=True)

    fields_out, spectra_out, gradient = pl.pallas_call(
        functools.partial(finish, groups, freqs, count),
        out_shape=[
            f32(NFIELD, 2, LANES),
            f32(freqs * PARTS * rows_all, LANES),
            f32(1, LANES),
        ],
        in_specs=[whole()] * 3,
        out_specs=[whole(pl.ANY)] * 3,
        scratch_shapes=[
            VMEM((members * MSG_ROWS, LANES), jnp.float32),
            VMEM(((2 * NFIELD + NPROP) * rows_all, LANES), jnp.float32),
            VMEM((2 * rows_all, LANES), jnp.float32),
            VMEM((2, STEPS * rows_all, 2 * LANES), jnp.float32),
            VMEM((2 * STEPS, LANES), jnp.float32),
            VMEM((1, LANES), jnp.float32),
            VMEM((2 * STEPS * 2 * rows_all, LANES), jnp.float32),
            VMEM((2, NFIELD, rows_all, LANES), jnp.float32),
            VMEM((2, STEPS, 2 * LANES), jnp.float32),
            VMEM((NFIELD, 2, LANES), jnp.float32),
            VMEM((1, LANES), jnp.float32),
            VMEM((freqs * PARTS * rows_all, LANES), jnp.float32),
            pltpu.SemaphoreType.DMA((6,)),
        ],
        cost_estimate=cost(20_000_000, 2_000_000),
        compiler_params=params(4096),
        name="finish",
    )(received, kron, held)
    return fields_out[None], spectra_out.reshape(spectra.shape), gradient


def solution(mesh):
    return jax.shard_map(
        program,
        mesh=mesh,
        in_specs=(
            P("role", None, "freq", "space"),
            P("role", "freq", None, None, "space"),
            P("freq"),
            P("freq"),
            P("freq", "space"),
            P(),
            P("role", None),
            P("role", None, None),
        ),
        out_specs=(
            P("role", None, "freq", "space"),
            P("role", "freq", None, None, "space"),
            P(("role", "freq"), "space"),
        ),
        check_vma=False,
    )
```

```python
import functools

import jax
import jax.numpy as jnp
from jax import lax
from jax.experimental import pallas as pl
from jax.experimental.pallas import tpu as pltpu
from jax.sharding import PartitionSpec as P


F = 128
STEPS = 8
PERIOD = 64
NMAT = 8
NFIELD = 5
NPROP = 3
COURANT = 0.18
TWO_PI = 6.283185307179586
LANES = 128
HALO = STEPS
PARTS = 4
CHANNELS = NFIELD + 1
ROW_IDS = 2 * NFIELD
ROW_HALO = 2 * CHANNELS
ROW_LISTS = 14
ROW_WAVELET = 15
MSG_ROWS = 16
LIST = 16
AT_CELL_ROW, AT_CELL_COLUMN, AT_INDEX, AT_WEIGHT = (LIST * slot for slot in range(4))
VMEM = pltpu.VMEM


def whole(space=VMEM):
    return pl.BlockSpec(memory_space=space)


def cost(flops, read):
    return pl.CostEstimate(flops=flops, bytes_accessed=read, transcendentals=0)


def params(kib):
    return pltpu.CompilerParams(vmem_limit_bytes=kib * 1024)


def lane_ids(shape):
    return lax.broadcasted_iota(jnp.int32, shape, len(shape) - 1)


def is_even():
    return lax.rem(lax.axis_index("space"), 2) == 0


def pack_block(
    width_all,
    fields_in,
    ids_in,
    material_in,
    cells_in,
    index_in,
    weight_in,
    wavelets_in,
    spectra_in,
    block,
    edge_chip,
    edge_link,
    spectra,
    shades,
    fields,
    ids,
    material,
    cells,
    index,
    weight,
    wavelets,
    wide,
    sems,
):
    sources = (fields_in, ids_in, material_in, cells_in, index_in, weight_in, wavelets_in, spectra_in)
    targets = (fields, ids, material, cells, index, weight, wavelets, spectra)
    copies = [
        pltpu.make_async_copy(source, target, sems.at[slot])
        for slot, (source, target) in enumerate(zip(sources, targets))
    ]
    for copy in copies:
        copy.start()
    block[...] = jnp.zeros_like(block)
    wide[...] = jnp.zeros_like(wide)
    for copy in copies[:-1]:
        copy.wait()
    for field in range(NFIELD):
        block[2 * field : 2 * field + 2, :] = fields[field]
    block[ROW_IDS : ROW_IDS + 2, :] = (ids[...] + 1).astype(jnp.float32)
    for prop in range(NPROP):
        for kind in range(NMAT):
            value = jnp.full((1, LANES), COURANT * material[prop, kind], jnp.float32)
            row = prop * NMAT + kind
            shades[row : row + 1, :] = value
    cell_row = lax.div(cells[...], width_all)
    cell_column = cells[...] - cell_row * width_all
    wide[:STEPS, :LIST] = wavelets[...]
    lists = (cell_row.astype(jnp.float32), cell_column.astype(jnp.float32))
    lists += (index[...].astype(jnp.float32), weight[...])
    for slot, value in enumerate(lists):
        wide[STEPS + slot : STEPS + slot + 1, :LIST] = value
    for row, first in ((ROW_WAVELET, 0), (ROW_LISTS, STEPS)):
        spread = pltpu.roll(wide[first : first + 8, :], 0, 1, stride=LIST, stride_axis=0)
        block[row : row + 1, :] = jnp.sum(spread, axis=0, keepdims=True)
    lanes = lane_ids((2, LANES))
    low = jnp.zeros((2, LANES), jnp.float32)
    high = jnp.zeros((2, LANES), jnp.float32)
    for slot in range(CHANNELS):
        value = block[2 * slot : 2 * slot + 2, :]
        left = jnp.where(lanes < HALO, value, 0.0)
        right = jnp.where(lanes >= LANES - HALO, value, 0.0)
        low = low + pltpu.roll(left, HALO * slot, 1)
        high = high + pltpu.roll(right, (HALO * slot + HALO) % LANES, 1)
    even = is_even()
    edge_chip[...] = jnp.where(even, high, low)
    edge_link[...] = jnp.where(even, low, high)
    copies[-1].wait()


def pack_spectra(freqs, spectra, message):
    rows_all = message.shape[0]
    for row in range(rows_all):
        for part in range(PARTS):
            picked = spectra[pl.ds(part * rows_all + row, freqs, stride=PARTS * rows_all), :]
            message[row, part * freqs : (part + 1) * freqs, :] = picked.astype(jnp.bfloat16)


def pack_rows(block, from_chip, from_link, row_spectra, message, tile):
    even = is_even()
    before = jnp.where(even, from_link[...], from_chip[...])
    after = jnp.where(even, from_chip[...], from_link[...])
    tile[...] = block[...]
    tile[ROW_HALO : ROW_HALO + 2, :] = before + pltpu.roll(after, LANES // 2, 1)
    exact = tile[...]
    high = exact.astype(jnp.bfloat16).astype(jnp.float32)
    both = jnp.concatenate([high, exact - high], axis=0).astype(jnp.bfloat16)
    for row in range(message.shape[0]):
        message[row, : 2 * MSG_ROWS, :] = both
        message[row, 2 * MSG_ROWS :, :] = row_spectra[row]


def twiddle(freqs, block, kron):
    span = 8 * STEPS
    lanes = lax.broadcasted_iota(jnp.int32, (freqs, freqs), 1)
    rows = lax.broadcasted_iota(jnp.int32, (freqs, freqs), 0)
    index = pltpu.roll(block[ROW_LISTS : ROW_LISTS + 1, :], LANES - AT_INDEX, 1)[:, :freqs]
    diagonal = jnp.where(lanes == rows, index, 0.0)
    column = jnp.sum(diagonal, axis=1, keepdims=True).astype(jnp.int32)
    across = lax.bitwise_and(lane_ids((freqs, 2 * span)), span - 1)
    turns = lax.bitwise_and(column * lax.shift_right_logical(across, 3), PERIOD - 1)
    angle = turns.astype(jnp.float32) * (TWO_PI / PERIOD)
    upper = lane_ids((freqs, 2 * span)) >= span
    value = jnp.where(upper, -jnp.sin(angle), jnp.cos(angle))
    keep = lax.bitwise_and(lane_ids((8, span)), 7) == lax.broadcasted_iota(
        jnp.int32, (8, span), 0
    )
    for freq in range(freqs):
        pair = []
        for phase in range(2):
            one = value[freq : freq + 1, phase * span : (phase + 1) * span]
            pair.append(jnp.where(keep, jnp.broadcast_to(one, (8, span)), 0.0))
        kron[freq * 16 : (freq + 1) * 16, :] = jnp.concatenate(pair, axis=0).astype(jnp.bfloat16)


def unpack(groups, received, decoded, center, halos):
    rows_all = 2 * groups
    for source in range(2 * groups):
        both = received[source, : 2 * MSG_ROWS, :].astype(jnp.float32)
        decoded[source * MSG_ROWS : (source + 1) * MSG_ROWS, :] = (
            both[:MSG_ROWS, :] + both[MSG_ROWS:, :]
        )

    def gather(target, at, role, first):
        for k in range(2):
            start = role * groups * MSG_ROWS + first + k
            target[pl.ds(at + k, groups, stride=2), :] = decoded[
                pl.ds(start, groups, stride=MSG_ROWS), :
            ]

    for role in range(2):
        for field in range(NFIELD):
            gather(center, (role * NFIELD + field) * rows_all, role, 2 * field)
        gather(halos, role * rows_all, role, ROW_HALO)
    gather(center, 2 * NFIELD * rows_all, 0, ROW_IDS)


def prepare(groups, count, decoded, inject, table, weights):
    rows_all = 2 * groups
    first_column = lax.axis_index("space") * LANES

    def joined(first):
        value = decoded[pl.ds(ROW_LISTS, groups, stride=MSG_ROWS), :]
        value = pltpu.roll(value, LANES - first, 1)
        value = jnp.where(lane_ids((groups, LANES)) < LIST, value, 0.0)
        spread = pltpu.roll(value, 0, 1, stride=LIST, stride_axis=0)
        return jnp.sum(spread, axis=0, keepdims=True)

    weights[...] = joined(AT_WEIGHT)
    index = joined(AT_INDEX).astype(jnp.int32)
    times = lax.broadcasted_iota(jnp.int32, (STEPS, LANES), 0)
    turns = lax.bitwise_and(index * times, PERIOD - 1)
    angle = turns.astype(jnp.float32) * (TWO_PI / PERIOD)
    table[:STEPS, :] = jnp.cos(angle)
    table[STEPS:, :] = -jnp.sin(angle)
    window = lax.broadcasted_iota(jnp.int32, (2 * LANES, LANES), 0)
    window = jnp.where(window < LANES + LANES // 2, window, window - 2 * LANES)
    row_ids = lax.broadcasted_iota(jnp.int32, (rows_all, LANES), 0)
    lanes = lane_ids((rows_all, LANES))
    row_lanes = lane_ids((1, LANES))

    def twice(row, first):
        value = pltpu.roll(row, (LANES - first) % LANES, 1)
        value = jnp.where(row_lanes < count, value, 0.0)
        return value + pltpu.roll(value, count, 1)

    for role in range(2):
        base = role * groups * MSG_ROWS
        lists = decoded[base + ROW_LISTS : base + ROW_LISTS + 1, :]
        cell_row = twice(lists, AT_CELL_ROW)
        cell_column = twice(lists, AT_CELL_COLUMN)
        near = cell_column.astype(jnp.int32) - first_column
        hit_column = jnp.where(window == near, 1.0, 0.0).astype(jnp.bfloat16)
        hit_row = jnp.logical_and(row_ids == cell_row.astype(jnp.int32), lanes < 2 * count)
        exact = decoded[base + ROW_WAVELET : base + ROW_WAVELET + 1, :]
        high = exact.astype(jnp.bfloat16).astype(jnp.float32)
        low = exact - high
        terms = []
        for tick in range(STEPS):
            first = pltpu.roll(high, (LANES - tick * count) % LANES, 1)
            second = pltpu.roll(low, (LANES + count - tick * count) % LANES, 1)
            amount = jnp.where(row_lanes < count, first, second)
            terms.append(jnp.where(hit_row, jnp.broadcast_to(amount, (rows_all, LANES)), 0.0))
        left = jnp.concatenate(terms, axis=0).astype(jnp.bfloat16)
        inject[role] = lax.dot_general(
            left, hit_column, (((1,), (1,)), ((), ())), preferred_element_type=jnp.float32
        )


def step_fields(groups, center, halos, shades, inject, snaps, finals):
    rows_all = 2 * groups
    lanes = lane_ids((rows_all, LANES))
    row_ids = lax.broadcasted_iota(jnp.int32, (rows_all, 2 * LANES), 0)

    def extended(at, role, slot):
        middle = center[at * rows_all : (at + 1) * rows_all, :]
        halo = halos[role * rows_all : (role + 1) * rows_all, :]
        after = pltpu.roll(halo, (LANES + LANES // 2 - HALO * slot) % LANES, 1)
        before = pltpu.roll(halo, (2 * LANES - HALO - HALO * slot) % LANES, 1)
        side = jnp.where(lanes < HALO, after, jnp.where(lanes >= LANES - HALO, before, 0.0))
        return jnp.concatenate([middle, side], axis=1)

    def up(value):
        return jnp.where(row_ids < rows_all - 1, pltpu.roll(value, rows_all - 1, 0), 0.0)

    def down(value):
        return jnp.where(row_ids > 0, pltpu.roll(value, 1, 0), 0.0)

    def after(value):
        return pltpu.roll(value, 2 * LANES - 1, 1)

    def before(value):
        return pltpu.roll(value, 1, 1)

    which = extended(2 * NFIELD, 0, NFIELD)
    props = []
    for prop in range(NPROP):
        value = jnp.zeros_like(which)
        for kind in range(NMAT):
            row = prop * NMAT + kind
            shade = shades[row : row + 1, :]
            shade = jnp.broadcast_to(jnp.concatenate([shade, shade], axis=1), which.shape)
            value = jnp.where(which == kind + 1.0, shade, value)
        props.append(value)
    buoyancy, lame_first, lame_second = props
    stiff = lame_first + 2.0 * lame_second
    for role in range(2):
        vel_x, vel_z, sig_xx, sig_zz, sig_xz = (
            extended(role * NFIELD + field, role, field) for field in range(NFIELD)
        )
        for tick in range(STEPS):
            vel_x = vel_x + buoyancy * ((up(sig_xx) - sig_xx) + (sig_xz - before(sig_xz)))
            vel_z = vel_z + buoyancy * ((sig_xz - down(sig_xz)) + (after(sig_zz) - sig_zz))
            source = inject[role, tick * rows_all : (tick + 1) * rows_all, :]
            strain_x = vel_x - down(vel_x)
            strain_z = vel_z - before(vel_z)
            sig_xx = sig_xx + (stiff * strain_x + lame_first * strain_z) + source
            sig_zz = sig_zz + (lame_first * strain_x + stiff * strain_z) + source
            sig_xz = sig_xz + lame_second * ((after(vel_x) - vel_x) + (up(vel_z) - vel_z))
            for part, value in enumerate((vel_x, vel_z)):
                at = ((role * STEPS + tick) * 2 + part) * rows_all
                rounded = value[:, :LANES].astype(jnp.bfloat16).astype(jnp.float32)
                snaps[at : at + rows_all, :] = rounded
        for field, value in enumerate((vel_x, vel_z, sig_xx, sig_zz, sig_xz)):
            finals[role, field] = value[:, :LANES]


def correlate(groups, freqs, received, row_snaps, table, weights, gradient):
    turned = table[...].astype(jnp.bfloat16)
    added = []
    for role in range(2):
        right = row_snaps[role].astype(jnp.bfloat16)
        phases = []
        for phase in range(2):
            phases.append(
                lax.dot_general(
                    turned[phase * STEPS : (phase + 1) * STEPS, :],
                    right,
                    (((0,), (0,)), ((), ())),
                    preferred_element_type=jnp.float32,
                )
            )
        added.append(phases)
    total = None
    for part in range(PARTS):
        sides = []
        first = 2 * MSG_ROWS + part * freqs
        for role in range(2):
            pieces = [
                received[role * groups + group, first : first + freqs, :]
                for group in range(groups)
            ]
            column = (part % 2) * LANES
            own = added[role][part // 2][:, column : column + LANES]
            sides.append(jnp.concatenate(pieces, axis=0).astype(jnp.float32) + own)
        product = sides[0] * sides[1]
        total = product if total is None else total + product
    gradient[...] = (
        lax.dot_general(
            weights[...],
            total,
            (((1,), (0,)), ((), ())),
            precision=lax.Precision.HIGHEST,
            preferred_element_type=jnp.float32,
        )
        * (1.0 / F)
    )


def finish(
    groups,
    freqs,
    count,
    received,
    kron,
    spectra,
    shades,
    fields_out,
    spectra_out,
    gradient_out,
    decoded,
    center,
    halos,
    inject,
    table,
    weights,
    snaps,
    finals,
    row_snaps,
    own_fields,
    gradient,
    held,
    sems,
):
    rows_all = 2 * groups
    own_role = lax.axis_index("role")
    own_group = lax.axis_index("freq")
    unpack(groups, received, decoded, center, halos)
    prepare(groups, count, decoded, inject, table, weights)
    step_fields(groups, center, halos, shades, inject, snaps, finals)
    for field in range(NFIELD):
        own_fields[field] = finals[own_role, field, pl.ds(2 * own_group, 2), :]
    copies = [pltpu.make_async_copy(own_fields, fields_out, sems.at[0])]
    copies[0].start()
    base = own_role * (STEPS * 2 * rows_all)
    blocks = []
    for part in range(2):
        for half in range(rows_all // 8):
            pieces = [
                snaps[pl.ds(pl.multiple_of(base + (tick * 2 + part) * rows_all + half * 8, 8), 8), :]
                for tick in range(STEPS)
            ]
            blocks.append(jnp.concatenate(pieces, axis=0))
    right = jnp.concatenate(blocks, axis=1).astype(jnp.bfloat16)
    per_freq = PARTS * rows_all
    chunk = freqs // 4
    for step in range(4):
        added = lax.dot_general(
            kron[step * chunk * 16 : (step + 1) * chunk * 16, :],
            right,
            (((1,), (0,)), ((), ())),
            preferred_element_type=jnp.float32,
        )
        for freq in range(chunk):
            for phase in range(2):
                for part in range(2):
                    for half in range(rows_all // 8):
                        at = (step * chunk + freq) * per_freq
                        at = at + (phase * 2 + part) * rows_all + half * 8
                        row = (freq * 2 + phase) * 8
                        column = (part * (rows_all // 8) + half) * LANES
                        held[at : at + 8, :] = (
                            spectra[at : at + 8, :]
                            + added[row : row + 8, column : column + LANES]
                        )
        span = pl.ds(step * chunk * per_freq, chunk * per_freq)
        copy = pltpu.make_async_copy(held.at[span], spectra_out.at[span], sems.at[1 + step])
        copy.start()
        copies.append(copy)
    own_row = own_role * groups + own_group
    for role in range(2):
        for part in range(2):
            start = (role * STEPS * 2 + part) * rows_all + own_row
            row_snaps[role, :, part * LANES : (part + 1) * LANES] = snaps[
                pl.ds(start, STEPS, stride=2 * rows_all), :
            ]
    correlate(groups, freqs, received, row_snaps, table, weights, gradient)
    copy = pltpu.make_async_copy(gradient, gradient_out, sems.at[5])
    copy.start()
    copies.append(copy)
    for copy in copies:
        copy.wait()


def f32(*shape):
    return jax.ShapeDtypeStruct(shape, jnp.float32)


def in_hbm(*arrays):
    return [pltpu.with_memory_space_constraint(array, pltpu.HBM) for array in arrays]


def swaps(size, first):
    pairs = [(i, i + 1) for i in range(first, size - 1, 2)]
    return pairs + [(b, a) for a, b in pairs]


def program(fields, spectra, freq_index, freq_weight, material_ids, material, source_cells, wavelets):
    groups = lax.axis_size("freq")
    members = 2 * groups
    freqs = freq_index.shape[0]
    rows_all = 2 * groups
    count = source_cells.shape[1]
    size = lax.axis_size("space")
    flat = spectra.reshape(freqs * PARTS * rows_all, LANES)
    message_rows = 2 * MSG_ROWS + PARTS * freqs

    block, edge_chip, edge_link, held, shades = pl.pallas_call(
        functools.partial(pack_block, LANES * size),
        out_shape=[
            VMEM((MSG_ROWS, LANES), jnp.float32),
            VMEM((2, LANES), jnp.float32),
            VMEM((2, LANES), jnp.float32),
            VMEM(flat.shape, jnp.float32),
            VMEM((NPROP * NMAT, LANES), jnp.float32),
        ],
        in_specs=[whole(pl.ANY)] * 8,
        out_specs=[whole()] * 5,
        scratch_shapes=[
            VMEM((NFIELD, 2, LANES), jnp.float32),
            VMEM((2, LANES), jnp.int32),
            pltpu.SMEM(material.shape, jnp.float32),
            VMEM((1, count), jnp.int32),
            VMEM((1, freqs), jnp.int32),
            VMEM((1, freqs), jnp.float32),
            VMEM((STEPS, count), jnp.float32),
            VMEM((2 * STEPS, LANES), jnp.float32),
            pltpu.SemaphoreType.DMA((8,)),
        ],
        cost_estimate=cost(100_000, 40_000),
        compiler_params=params(1024),
        name="pack_block",
    )(
        *in_hbm(
            fields[0],
            material_ids,
            material,
            source_cells,
            freq_index[None],
            freq_weight[None],
            wavelets[0],
            flat,
        )
    )
    from_link = lax.ppermute(edge_link, "space", swaps(size, 1))
    from_chip = lax.ppermute(edge_chip, "space", swaps(size, 0))

    kron = pl.pallas_call(
        functools.partial(twiddle, freqs),
        out_shape=jax.ShapeDtypeStruct((freqs * 16, STEPS * 8), jnp.bfloat16),
        in_specs=[whole()],
        out_specs=whole(),
        cost_estimate=cost(100_000, 40_000),
        compiler_params=params(512),
        name="twiddle",
    )(block)

    row_spectra = pl.pallas_call(
        functools.partial(pack_spectra, freqs),
        out_shape=VMEM((members, PARTS * freqs, LANES), jnp.bfloat16),
        in_specs=[whole()],
        out_specs=whole(),
        cost_estimate=cost(2_000_000, 1_000_000),
        compiler_params=params(1536),
        name="pack_spectra",
    )(held)
    message = pl.pallas_call(
        pack_rows,
        out_shape=VMEM((members, message_rows, LANES), jnp.bfloat16),
        in_specs=[whole()] * 4,
        out_specs=whole(),
        scratch_shapes=[VMEM((MSG_ROWS, LANES), jnp.float32)],
        cost_estimate=cost(100_000, 300_000),
        compiler_params=params(2048),
        name="pack_rows",
    )(block, from_chip, from_link, row_spectra)
    received = lax.all_to_all(message, ("role", "freq"), 0, 0, tiled=True)

    fields_out, spectra_out, gradient = pl.pallas_call(
        functools.partial(finish, groups, freqs, count),
        out_shape=[
            f32(NFIELD, 2, LANES),
            f32(freqs * PARTS * rows_all, LANES),
            f32(1, LANES),
        ],
        in_specs=[whole()] * 4,
        out_specs=[whole(pl.ANY)] * 3,
        scratch_shapes=[
            VMEM((members * MSG_ROWS, LANES), jnp.float32),
            VMEM(((2 * NFIELD + 1) * rows_all, LANES), jnp.float32),
            VMEM((2 * rows_all, LANES), jnp.float32),
            VMEM((2, STEPS * rows_all, 2 * LANES), jnp.float32),
            VMEM((2 * STEPS, LANES), jnp.float32),
            VMEM((1, LANES), jnp.float32),
            VMEM((2 * STEPS * 2 * rows_all, LANES), jnp.float32),
            VMEM((2, NFIELD, rows_all, LANES), jnp.float32),
            VMEM((2, STEPS, 2 * LANES), jnp.float32),
            VMEM((NFIELD, 2, LANES), jnp.float32),
            VMEM((1, LANES), jnp.float32),
            VMEM((freqs * PARTS * rows_all, LANES), jnp.float32),
            pltpu.SemaphoreType.DMA((6,)),
        ],
        cost_estimate=cost(20_000_000, 2_000_000),
        compiler_params=params(4096),
        name="finish",
    )(received, kron, held, shades)
    return fields_out[None], spectra_out.reshape(spectra.shape), gradient


def solution(mesh):
    return jax.shard_map(
        program,
        mesh=mesh,
        in_specs=(
            P("role", None, "freq", "space"),
            P("role", "freq", None, None, "space"),
            P("freq"),
            P("freq"),
            P("freq", "space"),
            P(),
            P("role", None),
            P("role", None, None),
        ),
        out_specs=(
            P("role", None, "freq", "space"),
            P("role", "freq", None, None, "space"),
            P(("role", "freq"), "space"),
        ),
        check_vma=False,
    )
```

```python
import functools

import jax
import jax.numpy as jnp
from jax import lax
from jax.experimental import pallas as pl
from jax.experimental.pallas import tpu as pltpu
from jax.sharding import PartitionSpec as P


F = 128
STEPS = 8
PERIOD = 64
NMAT = 8
NFIELD = 5
NPROP = 3
COURANT = 0.18
TWO_PI = 6.283185307179586
LANES = 128
HALO = STEPS
PARTS = 4
CHANNELS = NFIELD + 1
ROW_IDS = 2 * NFIELD
ROW_HALO = 2 * CHANNELS
ROW_LISTS = 14
ROW_WAVELET = 15
MSG_ROWS = 16
LIST = 16
AT_CELL_ROW, AT_CELL_COLUMN, AT_INDEX, AT_WEIGHT = (LIST * slot for slot in range(4))
VMEM = pltpu.VMEM


def whole(space=VMEM):
    return pl.BlockSpec(memory_space=space)


def cost(flops, read):
    return pl.CostEstimate(flops=flops, bytes_accessed=read, transcendentals=0)


def params(kib):
    return pltpu.CompilerParams(vmem_limit_bytes=kib * 1024)


def lane_ids(shape):
    return lax.broadcasted_iota(jnp.int32, shape, len(shape) - 1)


def is_even():
    return lax.rem(lax.axis_index("space"), 2) == 0


def pack_block(
    width_all,
    fields_in,
    ids_in,
    material_in,
    cells_in,
    index_in,
    weight_in,
    wavelets_in,
    spectra_in,
    block,
    edge_chip,
    edge_link,
    spectra,
    shades,
    fields,
    ids,
    material,
    cells,
    index,
    weight,
    wavelets,
    wide,
    sems,
):
    sources = (fields_in, ids_in, material_in, cells_in, index_in, weight_in, wavelets_in, spectra_in)
    targets = (fields, ids, material, cells, index, weight, wavelets, spectra)
    copies = [
        pltpu.make_async_copy(source, target, sems.at[slot])
        for slot, (source, target) in enumerate(zip(sources, targets))
    ]
    for copy in copies:
        copy.start()
    block[...] = jnp.zeros_like(block)
    wide[...] = jnp.zeros_like(wide)
    for copy in copies[:-1]:
        copy.wait()
    for field in range(NFIELD):
        block[2 * field : 2 * field + 2, :] = fields[field]
    block[ROW_IDS : ROW_IDS + 2, :] = (ids[...] + 1).astype(jnp.float32)
    for prop in range(NPROP):
        for kind in range(NMAT):
            value = jnp.full((1, LANES), COURANT * material[prop, kind], jnp.float32)
            row = prop * NMAT + kind
            shades[row : row + 1, :] = value
    cell_row = lax.div(cells[...], width_all)
    cell_column = cells[...] - cell_row * width_all
    wide[:STEPS, :LIST] = wavelets[...]
    lists = (cell_row.astype(jnp.float32), cell_column.astype(jnp.float32))
    lists += (index[...].astype(jnp.float32), weight[...])
    for slot, value in enumerate(lists):
        wide[STEPS + slot : STEPS + slot + 1, :LIST] = value
    for row, first in ((ROW_WAVELET, 0), (ROW_LISTS, STEPS)):
        spread = pltpu.roll(wide[first : first + 8, :], 0, 1, stride=LIST, stride_axis=0)
        block[row : row + 1, :] = jnp.sum(spread, axis=0, keepdims=True)
    lanes = lane_ids((2, LANES))
    low = jnp.zeros((2, LANES), jnp.float32)
    high = jnp.zeros((2, LANES), jnp.float32)
    for slot in range(CHANNELS):
        value = block[2 * slot : 2 * slot + 2, :]
        left = jnp.where(lanes < HALO, value, 0.0)
        right = jnp.where(lanes >= LANES - HALO, value, 0.0)
        low = low + pltpu.roll(left, HALO * slot, 1)
        high = high + pltpu.roll(right, (HALO * slot + HALO) % LANES, 1)
    even = is_even()
    edge_chip[...] = jnp.where(even, high, low)
    edge_link[...] = jnp.where(even, low, high)
    copies[-1].wait()


def pack_spectra(freqs, spectra, message):
    rows_all = message.shape[0]
    for row in range(rows_all):
        for part in range(PARTS):
            picked = spectra[pl.ds(part * rows_all + row, freqs, stride=PARTS * rows_all), :]
            message[row, part * freqs : (part + 1) * freqs, :] = picked.astype(jnp.bfloat16)


def pack_rows(block, from_chip, from_link, row_spectra, message, tile):
    even = is_even()
    before = jnp.where(even, from_link[...], from_chip[...])
    after = jnp.where(even, from_chip[...], from_link[...])
    tile[...] = block[...]
    tile[ROW_HALO : ROW_HALO + 2, :] = before + pltpu.roll(after, LANES // 2, 1)
    exact = tile[...]
    high = exact.astype(jnp.bfloat16).astype(jnp.float32)
    both = jnp.concatenate([high, exact - high], axis=0).astype(jnp.bfloat16)
    for row in range(message.shape[0]):
        message[row, : 2 * MSG_ROWS, :] = both
        message[row, 2 * MSG_ROWS :, :] = row_spectra[row]


def twiddle(freqs, block, kron):
    span = 8 * STEPS
    lanes = lax.broadcasted_iota(jnp.int32, (freqs, freqs), 1)
    rows = lax.broadcasted_iota(jnp.int32, (freqs, freqs), 0)
    index = pltpu.roll(block[ROW_LISTS : ROW_LISTS + 1, :], LANES - AT_INDEX, 1)[:, :freqs]
    diagonal = jnp.where(lanes == rows, index, 0.0)
    column = jnp.sum(diagonal, axis=1, keepdims=True).astype(jnp.int32)
    across = lax.bitwise_and(lane_ids((freqs, 2 * span)), span - 1)
    turns = lax.bitwise_and(column * lax.shift_right_logical(across, 3), PERIOD - 1)
    angle = turns.astype(jnp.float32) * (TWO_PI / PERIOD)
    upper = lane_ids((freqs, 2 * span)) >= span
    value = jnp.where(upper, -jnp.sin(angle), jnp.cos(angle))
    keep = lax.bitwise_and(lane_ids((8, span)), 7) == lax.broadcasted_iota(
        jnp.int32, (8, span), 0
    )
    for freq in range(freqs):
        pair = []
        for phase in range(2):
            one = value[freq : freq + 1, phase * span : (phase + 1) * span]
            pair.append(jnp.where(keep, jnp.broadcast_to(one, (8, span)), 0.0))
        kron[freq * 16 : (freq + 1) * 16, :] = jnp.concatenate(pair, axis=0).astype(jnp.bfloat16)


def unpack(groups, received, decoded, center, halos):
    rows_all = 2 * groups
    for source in range(2 * groups):
        both = received[source, : 2 * MSG_ROWS, :].astype(jnp.float32)
        decoded[source * MSG_ROWS : (source + 1) * MSG_ROWS, :] = (
            both[:MSG_ROWS, :] + both[MSG_ROWS:, :]
        )

    def gather(target, at, role, first):
        for k in range(2):
            start = role * groups * MSG_ROWS + first + k
            target[at + k * groups : at + (k + 1) * groups, :] = decoded[
                pl.ds(start, groups, stride=MSG_ROWS), :
            ]

    for role in range(2):
        for field in range(NFIELD):
            gather(center, (role * NFIELD + field) * rows_all, role, 2 * field)
        gather(halos, role * rows_all, role, ROW_HALO)
    gather(center, 2 * NFIELD * rows_all, 0, ROW_IDS)


def prepare(groups, count, decoded, inject, table, weights):
    rows_all = 2 * groups
    first_column = lax.axis_index("space") * LANES

    def joined(first):
        value = decoded[pl.ds(ROW_LISTS, groups, stride=MSG_ROWS), :]
        value = pltpu.roll(value, LANES - first, 1)
        value = jnp.where(lane_ids((groups, LANES)) < LIST, value, 0.0)
        spread = pltpu.roll(value, 0, 1, stride=LIST, stride_axis=0)
        return jnp.sum(spread, axis=0, keepdims=True)

    weights[...] = joined(AT_WEIGHT)
    index = joined(AT_INDEX).astype(jnp.int32)
    times = lax.broadcasted_iota(jnp.int32, (STEPS, LANES), 0)
    turns = lax.bitwise_and(index * times, PERIOD - 1)
    angle = turns.astype(jnp.float32) * (TWO_PI / PERIOD)
    table[:STEPS, :] = jnp.cos(angle)
    table[STEPS:, :] = -jnp.sin(angle)
    window = lax.broadcasted_iota(jnp.int32, (2 * LANES, LANES), 0)
    first_tile = jnp.where(window < LANES - HALO, window, window - LANES)
    second_tile = jnp.where(window < LANES + HALO, window, window - LANES)
    window = jnp.where(window < LANES, first_tile, second_tile)
    place = lax.broadcasted_iota(jnp.int32, (rows_all, LANES), 0)
    row_ids = jnp.where(place < groups, 2 * place, 2 * (place - groups) + 1)
    lanes = lane_ids((rows_all, LANES))
    row_lanes = lane_ids((1, LANES))

    def twice(row, first):
        value = pltpu.roll(row, (LANES - first) % LANES, 1)
        value = jnp.where(row_lanes < count, value, 0.0)
        return value + pltpu.roll(value, count, 1)

    for role in range(2):
        base = role * groups * MSG_ROWS
        lists = decoded[base + ROW_LISTS : base + ROW_LISTS + 1, :]
        cell_row = twice(lists, AT_CELL_ROW)
        cell_column = twice(lists, AT_CELL_COLUMN)
        near = cell_column.astype(jnp.int32) - first_column
        hit_column = jnp.where(window == near, 1.0, 0.0).astype(jnp.bfloat16)
        hit_row = jnp.logical_and(row_ids == cell_row.astype(jnp.int32), lanes < 2 * count)
        exact = decoded[base + ROW_WAVELET : base + ROW_WAVELET + 1, :]
        high = exact.astype(jnp.bfloat16).astype(jnp.float32)
        low = exact - high
        terms = []
        for tick in range(STEPS):
            first = pltpu.roll(high, (LANES - tick * count) % LANES, 1)
            second = pltpu.roll(low, (LANES + count - tick * count) % LANES, 1)
            amount = jnp.where(row_lanes < count, first, second)
            terms.append(jnp.where(hit_row, jnp.broadcast_to(amount, (rows_all, LANES)), 0.0))
        left = jnp.concatenate(terms, axis=0).astype(jnp.bfloat16)
        inject[role] = lax.dot_general(
            left, hit_column, (((1,), (1,)), ((), ())), preferred_element_type=jnp.float32
        )


def step_fields(groups, center, halos, shades, inject, snaps, finals):
    rows_all = 2 * groups
    lanes = lane_ids((rows_all, LANES))
    place = lax.broadcasted_iota(jnp.int32, (groups, LANES), 0)

    def extended(at, role, slot):
        middle = center[at * rows_all : (at + 1) * rows_all, :]
        halo = halos[role * rows_all : (role + 1) * rows_all, :]
        after = pltpu.roll(halo, (LANES + LANES // 2 - HALO * slot) % LANES, 1)
        before = pltpu.roll(halo, (2 * LANES - HALO - HALO * slot) % LANES, 1)
        first = jnp.where(lanes >= LANES - HALO, before, middle)
        second = jnp.where(lanes < HALO, after, middle)
        return jnp.concatenate([first, second], axis=0)

    def own(value):
        return jnp.where(lanes < LANES // 2, value[:rows_all, :], value[rows_all:, :])

    def up(value):
        parts = []
        for at in (0, rows_all):
            shifted = pltpu.roll(value[at : at + groups, :], groups - 1, 0)
            shifted = jnp.where(place < groups - 1, shifted, 0.0)
            parts += [value[at + groups : at + rows_all, :], shifted]
        return jnp.concatenate(parts, axis=0)

    def down(value):
        parts = []
        for at in (0, rows_all):
            shifted = pltpu.roll(value[at + groups : at + rows_all, :], 1, 0)
            shifted = jnp.where(place > 0, shifted, 0.0)
            parts += [shifted, value[at : at + groups, :]]
        return jnp.concatenate(parts, axis=0)

    def after(value):
        return pltpu.roll(value, LANES - 1, 1)

    def before(value):
        return pltpu.roll(value, 1, 1)

    which = extended(2 * NFIELD, 0, NFIELD)
    props = []
    for prop in range(NPROP):
        value = jnp.zeros_like(which)
        for kind in range(NMAT):
            row = prop * NMAT + kind
            shade = shades[row : row + 1, :]
            shade = jnp.broadcast_to(shade, which.shape)
            value = jnp.where(which == kind + 1.0, shade, value)
        props.append(value)
    buoyancy, lame_first, lame_second = props
    stiff = lame_first + 2.0 * lame_second
    states = [
        tuple(extended(role * NFIELD + field, role, field) for field in range(NFIELD))
        for role in range(2)
    ]
    for tick in range(STEPS):
        for role in range(2):
            vel_x, vel_z, sig_xx, sig_zz, sig_xz = states[role]
            vel_x = vel_x + buoyancy * ((up(sig_xx) - sig_xx) + (sig_xz - before(sig_xz)))
            vel_z = vel_z + buoyancy * ((sig_xz - down(sig_xz)) + (after(sig_zz) - sig_zz))
            for part, value in enumerate((vel_x, vel_z)):
                at = ((role * STEPS + tick) * 2 + part) * rows_all
                rounded = own(value).astype(jnp.bfloat16).astype(jnp.float32)
                for k in range(2):
                    half = rounded[k * groups : (k + 1) * groups, :]
                    snaps[pl.ds(at + k, groups, stride=2), :] = half
            states[role] = (vel_x, vel_z, sig_xx, sig_zz, sig_xz)
        for role in range(2):
            vel_x, vel_z, sig_xx, sig_zz, sig_xz = states[role]
            source = inject[role, tick * rows_all : (tick + 1) * rows_all, :]
            source = jnp.concatenate([source[:, :LANES], source[:, LANES:]], axis=0)
            strain_x = vel_x - down(vel_x)
            strain_z = vel_z - before(vel_z)
            sig_xx = sig_xx + (stiff * strain_x + lame_first * strain_z) + source
            sig_zz = sig_zz + (lame_first * strain_x + stiff * strain_z) + source
            sig_xz = sig_xz + lame_second * ((after(vel_x) - vel_x) + (up(vel_z) - vel_z))
            states[role] = (vel_x, vel_z, sig_xx, sig_zz, sig_xz)
    for role in range(2):
        for field in range(NFIELD):
            finals[role, field] = own(states[role][field])


def correlate(groups, freqs, received, row_snaps, table, weights, gradient):
    turned = table[...].astype(jnp.bfloat16)
    added = []
    for role in range(2):
        right = row_snaps[role].astype(jnp.bfloat16)
        phases = []
        for phase in range(2):
            phases.append(
                lax.dot_general(
                    turned[phase * STEPS : (phase + 1) * STEPS, :],
                    right,
                    (((0,), (0,)), ((), ())),
                    preferred_element_type=jnp.float32,
                )
            )
        added.append(phases)
    total = None
    for part in range(PARTS):
        sides = []
        first = 2 * MSG_ROWS + part * freqs
        for role in range(2):
            pieces = [
                received[role * groups + group, first : first + freqs, :]
                for group in range(groups)
            ]
            column = (part % 2) * LANES
            own = added[role][part // 2][:, column : column + LANES]
            sides.append(jnp.concatenate(pieces, axis=0).astype(jnp.float32) + own)
        product = sides[0] * sides[1]
        total = product if total is None else total + product
    gradient[...] = (
        lax.dot_general(
            weights[...],
            total,
            (((1,), (0,)), ((), ())),
            precision=lax.Precision.HIGHEST,
            preferred_element_type=jnp.float32,
        )
        * (1.0 / F)
    )


def finish(
    groups,
    freqs,
    count,
    received,
    kron,
    spectra,
    shades,
    fields_out,
    spectra_out,
    gradient_out,
    decoded,
    center,
    halos,
    inject,
    table,
    weights,
    snaps,
    finals,
    row_snaps,
    own_fields,
    gradient,
    held,
    sems,
):
    rows_all = 2 * groups
    own_role = lax.axis_index("role")
    own_group = lax.axis_index("freq")
    unpack(groups, received, decoded, center, halos)
    prepare(groups, count, decoded, inject, table, weights)
    step_fields(groups, center, halos, shades, inject, snaps, finals)
    for field in range(NFIELD):
        for k in range(2):
            own_fields[field, k : k + 1, :] = finals[
                own_role, field, pl.ds(own_group + k * groups, 1), :
            ]
    copies = [pltpu.make_async_copy(own_fields, fields_out, sems.at[0])]
    copies[0].start()
    base = own_role * (STEPS * 2 * rows_all)
    blocks = []
    for part in range(2):
        for half in range(rows_all // 8):
            pieces = [
                snaps[pl.ds(pl.multiple_of(base + (tick * 2 + part) * rows_all + half * 8, 8), 8), :]
                for tick in range(STEPS)
            ]
            blocks.append(jnp.concatenate(pieces, axis=0))
    right = jnp.concatenate(blocks, axis=1).astype(jnp.bfloat16)
    per_freq = PARTS * rows_all
    chunk = freqs // 4
    for step in range(4):
        added = lax.dot_general(
            kron[step * chunk * 16 : (step + 1) * chunk * 16, :],
            right,
            (((1,), (0,)), ((), ())),
            preferred_element_type=jnp.float32,
        )
        for freq in range(chunk):
            for phase in range(2):
                for part in range(2):
                    for half in range(rows_all // 8):
                        at = (step * chunk + freq) * per_freq
                        at = at + (phase * 2 + part) * rows_all + half * 8
                        row = (freq * 2 + phase) * 8
                        column = (part * (rows_all // 8) + half) * LANES
                        held[at : at + 8, :] = (
                            spectra[at : at + 8, :]
                            + added[row : row + 8, column : column + LANES]
                        )
        span = pl.ds(step * chunk * per_freq, chunk * per_freq)
        copy = pltpu.make_async_copy(held.at[span], spectra_out.at[span], sems.at[1 + step])
        copy.start()
        copies.append(copy)
    own_row = own_role * groups + own_group
    for role in range(2):
        for part in range(2):
            start = (role * STEPS * 2 + part) * rows_all + own_row
            row_snaps[role, :, part * LANES : (part + 1) * LANES] = snaps[
                pl.ds(start, STEPS, stride=2 * rows_all), :
            ]
    correlate(groups, freqs, received, row_snaps, table, weights, gradient)
    copy = pltpu.make_async_copy(gradient, gradient_out, sems.at[5])
    copy.start()
    copies.append(copy)
    for copy in copies:
        copy.wait()


def f32(*shape):
    return jax.ShapeDtypeStruct(shape, jnp.float32)


def in_hbm(*arrays):
    return [pltpu.with_memory_space_constraint(array, pltpu.HBM) for array in arrays]


def swaps(size, first):
    pairs = [(i, i + 1) for i in range(first, size - 1, 2)]
    return pairs + [(b, a) for a, b in pairs]


def program(fields, spectra, freq_index, freq_weight, material_ids, material, source_cells, wavelets):
    groups = lax.axis_size("freq")
    members = 2 * groups
    freqs = freq_index.shape[0]
    rows_all = 2 * groups
    count = source_cells.shape[1]
    size = lax.axis_size("space")
    flat = spectra.reshape(freqs * PARTS * rows_all, LANES)
    message_rows = 2 * MSG_ROWS + PARTS * freqs

    block, edge_chip, edge_link, held, shades = pl.pallas_call(
        functools.partial(pack_block, LANES * size),
        out_shape=[
            VMEM((MSG_ROWS, LANES), jnp.float32),
            VMEM((2, LANES), jnp.float32),
            VMEM((2, LANES), jnp.float32),
            VMEM(flat.shape, jnp.float32),
            VMEM((NPROP * NMAT, LANES), jnp.float32),
        ],
        in_specs=[whole(pl.ANY)] * 8,
        out_specs=[whole()] * 5,
        scratch_shapes=[
            VMEM((NFIELD, 2, LANES), jnp.float32),
            VMEM((2, LANES), jnp.int32),
            pltpu.SMEM(material.shape, jnp.float32),
            VMEM((1, count), jnp.int32),
            VMEM((1, freqs), jnp.int32),
            VMEM((1, freqs), jnp.float32),
            VMEM((STEPS, count), jnp.float32),
            VMEM((2 * STEPS, LANES), jnp.float32),
            pltpu.SemaphoreType.DMA((8,)),
        ],
        cost_estimate=cost(100_000, 40_000),
        compiler_params=params(1024),
        name="pack_block",
    )(
        *in_hbm(
            fields[0],
            material_ids,
            material,
            source_cells,
            freq_index[None],
            freq_weight[None],
            wavelets[0],
            flat,
        )
    )
    from_link = lax.ppermute(edge_link, "space", swaps(size, 1))
    from_chip = lax.ppermute(edge_chip, "space", swaps(size, 0))

    kron = pl.pallas_call(
        functools.partial(twiddle, freqs),
        out_shape=jax.ShapeDtypeStruct((freqs * 16, STEPS * 8), jnp.bfloat16),
        in_specs=[whole()],
        out_specs=whole(),
        cost_estimate=cost(100_000, 40_000),
        compiler_params=params(512),
        name="twiddle",
    )(block)

    row_spectra = pl.pallas_call(
        functools.partial(pack_spectra, freqs),
        out_shape=VMEM((members, PARTS * freqs, LANES), jnp.bfloat16),
        in_specs=[whole()],
        out_specs=whole(),
        cost_estimate=cost(2_000_000, 1_000_000),
        compiler_params=params(1536),
        name="pack_spectra",
    )(held)
    message = pl.pallas_call(
        pack_rows,
        out_shape=VMEM((members, message_rows, LANES), jnp.bfloat16),
        in_specs=[whole()] * 4,
        out_specs=whole(),
        scratch_shapes=[VMEM((MSG_ROWS, LANES), jnp.float32)],
        cost_estimate=cost(100_000, 300_000),
        compiler_params=params(2048),
        name="pack_rows",
    )(block, from_chip, from_link, row_spectra)
    received = lax.all_to_all(message, ("role", "freq"), 0, 0, tiled=True)

    fields_out, spectra_out, gradient = pl.pallas_call(
        functools.partial(finish, groups, freqs, count),
        out_shape=[
            f32(NFIELD, 2, LANES),
            f32(freqs * PARTS * rows_all, LANES),
            f32(1, LANES),
        ],
        in_specs=[whole()] * 4,
        out_specs=[whole(pl.ANY)] * 3,
        scratch_shapes=[
            VMEM((members * MSG_ROWS, LANES), jnp.float32),
            VMEM(((2 * NFIELD + 1) * rows_all, LANES), jnp.float32),
            VMEM((2 * rows_all, LANES), jnp.float32),
            VMEM((2, STEPS * rows_all, 2 * LANES), jnp.float32),
            VMEM((2 * STEPS, LANES), jnp.float32),
            VMEM((1, LANES), jnp.float32),
            VMEM((2 * STEPS * 2 * rows_all, LANES), jnp.float32),
            VMEM((2, NFIELD, rows_all, LANES), jnp.float32),
            VMEM((2, STEPS, 2 * LANES), jnp.float32),
            VMEM((NFIELD, 2, LANES), jnp.float32),
            VMEM((1, LANES), jnp.float32),
            VMEM((freqs * PARTS * rows_all, LANES), jnp.float32),
            pltpu.SemaphoreType.DMA((6,)),
        ],
        cost_estimate=cost(20_000_000, 2_000_000),
        compiler_params=params(4096),
        name="finish",
    )(received, kron, held, shades)
    return fields_out[None], spectra_out.reshape(spectra.shape), gradient


def solution(mesh):
    return jax.shard_map(
        program,
        mesh=mesh,
        in_specs=(
            P("role", None, "freq", "space"),
            P("role", "freq", None, None, "space"),
            P("freq"),
            P("freq"),
            P("freq", "space"),
            P(),
            P("role", None),
            P("role", None, None),
        ),
        out_specs=(
            P("role", None, "freq", "space"),
            P("role", "freq", None, None, "space"),
            P(("role", "freq"), "space"),
        ),
        check_vma=False,
    )
```

```python
import functools

import jax
import jax.numpy as jnp
from jax import lax
from jax.experimental import pallas as pl
from jax.experimental.pallas import tpu as pltpu
from jax.sharding import PartitionSpec as P


F = 128
STEPS = 8
PERIOD = 64
NMAT = 8
NFIELD = 5
NPROP = 3
COURANT = 0.18
TWO_PI = 6.283185307179586
LANES = 128
HALO = STEPS
PARTS = 4
CHANNELS = NFIELD + 1
ROW_IDS = 2 * NFIELD
ROW_HALO = 2 * CHANNELS
ROW_LISTS = 14
ROW_WAVELET = 15
MSG_ROWS = 16
LIST = 16
AT_CELL_ROW, AT_CELL_COLUMN, AT_INDEX, AT_WEIGHT = (LIST * slot for slot in range(4))
VMEM = pltpu.VMEM


def whole(space=VMEM):
    return pl.BlockSpec(memory_space=space)


def cost(flops, read):
    return pl.CostEstimate(flops=flops, bytes_accessed=read, transcendentals=0)


def params(kib):
    return pltpu.CompilerParams(vmem_limit_bytes=kib * 1024)


def lane_ids(shape):
    return lax.broadcasted_iota(jnp.int32, shape, len(shape) - 1)


def is_even():
    return lax.rem(lax.axis_index("space"), 2) == 0


def pack_block(
    width_all,
    fields_in,
    ids_in,
    material_in,
    cells_in,
    index_in,
    weight_in,
    wavelets_in,
    spectra_in,
    block,
    edge_chip,
    edge_link,
    spectra,
    shades,
    fields,
    ids,
    material,
    cells,
    index,
    weight,
    wavelets,
    wide,
    sems,
):
    sources = (fields_in, ids_in, material_in, cells_in, index_in, weight_in, wavelets_in, spectra_in)
    targets = (fields, ids, material, cells, index, weight, wavelets, spectra)
    copies = [
        pltpu.make_async_copy(source, target, sems.at[slot])
        for slot, (source, target) in enumerate(zip(sources, targets))
    ]
    for copy in copies:
        copy.start()
    block[...] = jnp.zeros_like(block)
    wide[...] = jnp.zeros_like(wide)
    for copy in copies[:-1]:
        copy.wait()
    for field in range(NFIELD):
        block[2 * field : 2 * field + 2, :] = fields[field]
    block[ROW_IDS : ROW_IDS + 2, :] = (ids[...] + 1).astype(jnp.float32)
    for prop in range(NPROP):
        for kind in range(NMAT):
            value = jnp.full((1, LANES), COURANT * material[prop, kind], jnp.float32)
            row = prop * NMAT + kind
            shades[row : row + 1, :] = value
    cell_row = lax.div(cells[...], width_all)
    cell_column = cells[...] - cell_row * width_all
    wide[:STEPS, :LIST] = wavelets[...]
    lists = (cell_row.astype(jnp.float32), cell_column.astype(jnp.float32))
    lists += (index[...].astype(jnp.float32), weight[...])
    for slot, value in enumerate(lists):
        wide[STEPS + slot : STEPS + slot + 1, :LIST] = value
    for row, first in ((ROW_WAVELET, 0), (ROW_LISTS, STEPS)):
        spread = pltpu.roll(wide[first : first + 8, :], 0, 1, stride=LIST, stride_axis=0)
        block[row : row + 1, :] = jnp.sum(spread, axis=0, keepdims=True)
    lanes = lane_ids((2, LANES))
    low = jnp.zeros((2, LANES), jnp.float32)
    high = jnp.zeros((2, LANES), jnp.float32)
    for slot in range(CHANNELS):
        value = block[2 * slot : 2 * slot + 2, :]
        left = jnp.where(lanes < HALO, value, 0.0)
        right = jnp.where(lanes >= LANES - HALO, value, 0.0)
        low = low + pltpu.roll(left, HALO * slot, 1)
        high = high + pltpu.roll(right, (HALO * slot + HALO) % LANES, 1)
    even = is_even()
    edge_chip[...] = jnp.where(even, high, low)
    edge_link[...] = jnp.where(even, low, high)
    copies[-1].wait()


def pack_spectra(freqs, spectra, message):
    rows_all = message.shape[0]
    for row in range(rows_all):
        for part in range(PARTS):
            picked = spectra[pl.ds(part * rows_all + row, freqs, stride=PARTS * rows_all), :]
            message[row, part * freqs : (part + 1) * freqs, :] = picked.astype(jnp.bfloat16)


def pack_rows(block, from_chip, from_link, row_spectra, message, tile):
    even = is_even()
    before = jnp.where(even, from_link[...], from_chip[...])
    after = jnp.where(even, from_chip[...], from_link[...])
    tile[...] = block[...]
    tile[ROW_HALO : ROW_HALO + 2, :] = before + pltpu.roll(after, LANES // 2, 1)
    exact = tile[...]
    high = exact.astype(jnp.bfloat16).astype(jnp.float32)
    both = jnp.concatenate([high, exact - high], axis=0).astype(jnp.bfloat16)
    for row in range(message.shape[0]):
        message[row, : 2 * MSG_ROWS, :] = both
        message[row, 2 * MSG_ROWS :, :] = row_spectra[row]


def twiddle(freqs, block, kron, waves):
    lane = lane_ids((STEPS, LANES)).astype(jnp.float32) * (TWO_PI / PERIOD)
    waves[:STEPS, :] = jnp.cos(lane)
    waves[STEPS:, :] = -jnp.sin(lane)
    span = 8 * STEPS
    lanes = lax.broadcasted_iota(jnp.int32, (freqs, freqs), 1)
    rows = lax.broadcasted_iota(jnp.int32, (freqs, freqs), 0)
    index = pltpu.roll(block[ROW_LISTS : ROW_LISTS + 1, :], LANES - AT_INDEX, 1)[:, :freqs]
    diagonal = jnp.where(lanes == rows, index, 0.0)
    column = jnp.sum(diagonal, axis=1, keepdims=True).astype(jnp.int32)
    across = lax.bitwise_and(lane_ids((freqs, 2 * span)), span - 1)
    turns = lax.bitwise_and(column * lax.shift_right_logical(across, 3), PERIOD - 1)
    angle = turns.astype(jnp.float32) * (TWO_PI / PERIOD)
    upper = lane_ids((freqs, 2 * span)) >= span
    value = jnp.where(upper, -jnp.sin(angle), jnp.cos(angle))
    keep = lax.bitwise_and(lane_ids((8, span)), 7) == lax.broadcasted_iota(
        jnp.int32, (8, span), 0
    )
    for freq in range(freqs):
        pair = []
        for phase in range(2):
            one = value[freq : freq + 1, phase * span : (phase + 1) * span]
            pair.append(jnp.where(keep, jnp.broadcast_to(one, (8, span)), 0.0))
        kron[freq * 16 : (freq + 1) * 16, :] = jnp.concatenate(pair, axis=0).astype(jnp.bfloat16)


def unpack(groups, received, decoded, center, halos):
    rows_all = 2 * groups
    for source in range(2 * groups):
        both = received[source, : 2 * MSG_ROWS, :].astype(jnp.float32)
        decoded[source * MSG_ROWS : (source + 1) * MSG_ROWS, :] = (
            both[:MSG_ROWS, :] + both[MSG_ROWS:, :]
        )

    def gather(target, at, role, first):
        for k in range(2):
            start = role * groups * MSG_ROWS + first + k
            target[at + k * groups : at + (k + 1) * groups, :] = decoded[
                pl.ds(start, groups, stride=MSG_ROWS), :
            ]

    for role in range(2):
        for field in range(NFIELD):
            gather(center, (role * NFIELD + field) * rows_all, role, 2 * field)
        gather(halos, role * rows_all, role, ROW_HALO)
    gather(center, 2 * NFIELD * rows_all, 0, ROW_IDS)


def prepare(groups, count, decoded, waves, inject, table, weights):
    rows_all = 2 * groups
    first_column = lax.axis_index("space") * LANES

    def joined(first):
        value = decoded[pl.ds(ROW_LISTS, groups, stride=MSG_ROWS), :]
        value = pltpu.roll(value, LANES - first, 1)
        value = jnp.where(lane_ids((groups, LANES)) < LIST, value, 0.0)
        spread = pltpu.roll(value, 0, 1, stride=LIST, stride_axis=0)
        return jnp.sum(spread, axis=0, keepdims=True)

    weights[...] = joined(AT_WEIGHT)
    index = joined(AT_INDEX).astype(jnp.int32)
    times = lax.broadcasted_iota(jnp.int32, (STEPS, LANES), 0)
    turns = lax.bitwise_and(index * times, PERIOD - 1)
    table[:STEPS, :] = jnp.take_along_axis(waves[:STEPS, :], turns, axis=1)
    table[STEPS:, :] = jnp.take_along_axis(waves[STEPS:, :], turns, axis=1)
    window = lax.broadcasted_iota(jnp.int32, (2 * LANES, LANES), 0)
    first_tile = jnp.where(window < LANES - HALO, window, window - LANES)
    second_tile = jnp.where(window < LANES + HALO, window, window - LANES)
    window = jnp.where(window < LANES, first_tile, second_tile)
    place = lax.broadcasted_iota(jnp.int32, (rows_all, LANES), 0)
    row_ids = jnp.where(place < groups, 2 * place, 2 * (place - groups) + 1)
    lanes = lane_ids((rows_all, LANES))
    row_lanes = lane_ids((1, LANES))

    def twice(row, first):
        value = pltpu.roll(row, (LANES - first) % LANES, 1)
        value = jnp.where(row_lanes < count, value, 0.0)
        return value + pltpu.roll(value, count, 1)

    for role in range(2):
        base = role * groups * MSG_ROWS
        lists = decoded[base + ROW_LISTS : base + ROW_LISTS + 1, :]
        cell_row = twice(lists, AT_CELL_ROW)
        cell_column = twice(lists, AT_CELL_COLUMN)
        near = cell_column.astype(jnp.int32) - first_column
        hit_column = jnp.where(window == near, 1.0, 0.0).astype(jnp.bfloat16)
        hit_row = jnp.logical_and(row_ids == cell_row.astype(jnp.int32), lanes < 2 * count)
        exact = decoded[base + ROW_WAVELET : base + ROW_WAVELET + 1, :]
        high = exact.astype(jnp.bfloat16).astype(jnp.float32)
        low = exact - high
        terms = []
        for tick in range(STEPS):
            first = pltpu.roll(high, (LANES - tick * count) % LANES, 1)
            second = pltpu.roll(low, (LANES + count - tick * count) % LANES, 1)
            amount = jnp.where(row_lanes < count, first, second)
            terms.append(jnp.where(hit_row, jnp.broadcast_to(amount, (rows_all, LANES)), 0.0))
        left = jnp.concatenate(terms, axis=0).astype(jnp.bfloat16)
        inject[role] = lax.dot_general(
            left, hit_column, (((1,), (1,)), ((), ())), preferred_element_type=jnp.float32
        )


def step_fields(groups, center, halos, shades, inject, snaps, finals):
    rows_all = 2 * groups
    lanes = lane_ids((rows_all, LANES))
    place = lax.broadcasted_iota(jnp.int32, (groups, LANES), 0)

    def extended(at, role, slot):
        middle = center[at * rows_all : (at + 1) * rows_all, :]
        halo = halos[role * rows_all : (role + 1) * rows_all, :]
        after = pltpu.roll(halo, (LANES + LANES // 2 - HALO * slot) % LANES, 1)
        before = pltpu.roll(halo, (2 * LANES - HALO - HALO * slot) % LANES, 1)
        first = jnp.where(lanes >= LANES - HALO, before, middle)
        second = jnp.where(lanes < HALO, after, middle)
        return jnp.concatenate([first, second], axis=0)

    def own(value):
        return jnp.where(lanes < LANES // 2, value[:rows_all, :], value[rows_all:, :])

    def up(value):
        parts = []
        for at in (0, rows_all):
            shifted = pltpu.roll(value[at : at + groups, :], groups - 1, 0)
            shifted = jnp.where(place < groups - 1, shifted, 0.0)
            parts += [value[at + groups : at + rows_all, :], shifted]
        return jnp.concatenate(parts, axis=0)

    def down(value):
        parts = []
        for at in (0, rows_all):
            shifted = pltpu.roll(value[at + groups : at + rows_all, :], 1, 0)
            shifted = jnp.where(place > 0, shifted, 0.0)
            parts += [shifted, value[at : at + groups, :]]
        return jnp.concatenate(parts, axis=0)

    def after(value):
        return pltpu.roll(value, LANES - 1, 1)

    def before(value):
        return pltpu.roll(value, 1, 1)

    which = extended(2 * NFIELD, 0, NFIELD)
    props = []
    for prop in range(NPROP):
        value = jnp.zeros_like(which)
        for kind in range(NMAT):
            row = prop * NMAT + kind
            shade = shades[row : row + 1, :]
            shade = jnp.broadcast_to(shade, which.shape)
            value = jnp.where(which == kind + 1.0, shade, value)
        props.append(value)
    buoyancy, lame_first, lame_second = props
    stiff = lame_first + 2.0 * lame_second
    states = [
        tuple(extended(role * NFIELD + field, role, field) for field in range(NFIELD))
        for role in range(2)
    ]
    for tick in range(STEPS):
        for role in range(2):
            vel_x, vel_z, sig_xx, sig_zz, sig_xz = states[role]
            vel_x = vel_x + buoyancy * ((up(sig_xx) - sig_xx) + (sig_xz - before(sig_xz)))
            vel_z = vel_z + buoyancy * ((sig_xz - down(sig_xz)) + (after(sig_zz) - sig_zz))
            for part, value in enumerate((vel_x, vel_z)):
                at = ((role * STEPS + tick) * 2 + part) * rows_all
                rounded = own(value).astype(jnp.bfloat16).astype(jnp.float32)
                for k in range(2):
                    half = rounded[k * groups : (k + 1) * groups, :]
                    snaps[pl.ds(at + k, groups, stride=2), :] = half
            states[role] = (vel_x, vel_z, sig_xx, sig_zz, sig_xz)
        for role in range(2):
            vel_x, vel_z, sig_xx, sig_zz, sig_xz = states[role]
            source = inject[role, tick * rows_all : (tick + 1) * rows_all, :]
            source = jnp.concatenate([source[:, :LANES], source[:, LANES:]], axis=0)
            strain_x = vel_x - down(vel_x)
            strain_z = vel_z - before(vel_z)
            sig_xx = sig_xx + (stiff * strain_x + lame_first * strain_z) + source
            sig_zz = sig_zz + (lame_first * strain_x + stiff * strain_z) + source
            sig_xz = sig_xz + lame_second * ((after(vel_x) - vel_x) + (up(vel_z) - vel_z))
            states[role] = (vel_x, vel_z, sig_xx, sig_zz, sig_xz)
    for role in range(2):
        for field in range(NFIELD):
            finals[role, field] = own(states[role][field])


def correlate(groups, freqs, received, row_snaps, table, weights, gradient):
    turned = table[...].astype(jnp.bfloat16)
    added = []
    for role in range(2):
        right = row_snaps[role].astype(jnp.bfloat16)
        phases = []
        for phase in range(2):
            phases.append(
                lax.dot_general(
                    turned[phase * STEPS : (phase + 1) * STEPS, :],
                    right,
                    (((0,), (0,)), ((), ())),
                    preferred_element_type=jnp.float32,
                )
            )
        added.append(phases)
    total = None
    for part in range(PARTS):
        sides = []
        first = 2 * MSG_ROWS + part * freqs
        for role in range(2):
            pieces = [
                received[role * groups + group, first : first + freqs, :]
                for group in range(groups)
            ]
            column = (part % 2) * LANES
            own = added[role][part // 2][:, column : column + LANES]
            sides.append(jnp.concatenate(pieces, axis=0).astype(jnp.float32) + own)
        product = sides[0] * sides[1]
        total = product if total is None else total + product
    gradient[...] = (
        lax.dot_general(
            weights[...],
            total,
            (((1,), (0,)), ((), ())),
            precision=lax.Precision.HIGHEST,
            preferred_element_type=jnp.float32,
        )
        * (1.0 / F)
    )


def finish(
    groups,
    freqs,
    count,
    received,
    kron,
    waves,
    spectra,
    shades,
    fields_out,
    spectra_out,
    gradient_out,
    decoded,
    center,
    halos,
    inject,
    table,
    weights,
    snaps,
    finals,
    row_snaps,
    own_fields,
    gradient,
    held,
    sems,
):
    rows_all = 2 * groups
    own_role = lax.axis_index("role")
    own_group = lax.axis_index("freq")
    unpack(groups, received, decoded, center, halos)
    prepare(groups, count, decoded, waves, inject, table, weights)
    step_fields(groups, center, halos, shades, inject, snaps, finals)
    for field in range(NFIELD):
        for k in range(2):
            own_fields[field, k : k + 1, :] = finals[
                own_role, field, pl.ds(own_group + k * groups, 1), :
            ]
    copies = [pltpu.make_async_copy(own_fields, fields_out, sems.at[0])]
    copies[0].start()
    base = own_role * (STEPS * 2 * rows_all)
    blocks = []
    for part in range(2):
        for half in range(rows_all // 8):
            pieces = [
                snaps[pl.ds(pl.multiple_of(base + (tick * 2 + part) * rows_all + half * 8, 8), 8), :]
                for tick in range(STEPS)
            ]
            blocks.append(jnp.concatenate(pieces, axis=0))
    right = jnp.concatenate(blocks, axis=1).astype(jnp.bfloat16)
    per_freq = PARTS * rows_all
    chunk = freqs // 4
    for step in range(4):
        added = lax.dot_general(
            kron[step * chunk * 16 : (step + 1) * chunk * 16, :],
            right,
            (((1,), (0,)), ((), ())),
            preferred_element_type=jnp.float32,
        )
        for freq in range(chunk):
            for phase in range(2):
                for part in range(2):
                    for half in range(rows_all // 8):
                        at = (step * chunk + freq) * per_freq
                        at = at + (phase * 2 + part) * rows_all + half * 8
                        row = (freq * 2 + phase) * 8
                        column = (part * (rows_all // 8) + half) * LANES
                        held[at : at + 8, :] = (
                            spectra[at : at + 8, :]
                            + added[row : row + 8, column : column + LANES]
                        )
        span = pl.ds(step * chunk * per_freq, chunk * per_freq)
        copy = pltpu.make_async_copy(held.at[span], spectra_out.at[span], sems.at[1 + step])
        copy.start()
        copies.append(copy)
    own_row = own_role * groups + own_group
    for role in range(2):
        for part in range(2):
            start = (role * STEPS * 2 + part) * rows_all + own_row
            row_snaps[role, :, part * LANES : (part + 1) * LANES] = snaps[
                pl.ds(start, STEPS, stride=2 * rows_all), :
            ]
    correlate(groups, freqs, received, row_snaps, table, weights, gradient)
    copy = pltpu.make_async_copy(gradient, gradient_out, sems.at[5])
    copy.start()
    copies.append(copy)
    for copy in copies:
        copy.wait()


def f32(*shape):
    return jax.ShapeDtypeStruct(shape, jnp.float32)


def in_hbm(*arrays):
    return [pltpu.with_memory_space_constraint(array, pltpu.HBM) for array in arrays]


def swaps(size, first):
    pairs = [(i, i + 1) for i in range(first, size - 1, 2)]
    return pairs + [(b, a) for a, b in pairs]


def program(fields, spectra, freq_index, freq_weight, material_ids, material, source_cells, wavelets):
    groups = lax.axis_size("freq")
    members = 2 * groups
    freqs = freq_index.shape[0]
    rows_all = 2 * groups
    count = source_cells.shape[1]
    size = lax.axis_size("space")
    flat = spectra.reshape(freqs * PARTS * rows_all, LANES)
    message_rows = 2 * MSG_ROWS + PARTS * freqs

    block, edge_chip, edge_link, held, shades = pl.pallas_call(
        functools.partial(pack_block, LANES * size),
        out_shape=[
            VMEM((MSG_ROWS, LANES), jnp.float32),
            VMEM((2, LANES), jnp.float32),
            VMEM((2, LANES), jnp.float32),
            VMEM(flat.shape, jnp.float32),
            VMEM((NPROP * NMAT, LANES), jnp.float32),
        ],
        in_specs=[whole(pl.ANY)] * 8,
        out_specs=[whole()] * 5,
        scratch_shapes=[
            VMEM((NFIELD, 2, LANES), jnp.float32),
            VMEM((2, LANES), jnp.int32),
            pltpu.SMEM(material.shape, jnp.float32),
            VMEM((1, count), jnp.int32),
            VMEM((1, freqs), jnp.int32),
            VMEM((1, freqs), jnp.float32),
            VMEM((STEPS, count), jnp.float32),
            VMEM((2 * STEPS, LANES), jnp.float32),
            pltpu.SemaphoreType.DMA((8,)),
        ],
        cost_estimate=cost(100_000, 40_000),
        compiler_params=params(1024),
        name="pack_block",
    )(
        *in_hbm(
            fields[0],
            material_ids,
            material,
            source_cells,
            freq_index[None],
            freq_weight[None],
            wavelets[0],
            flat,
        )
    )
    from_link = lax.ppermute(edge_link, "space", swaps(size, 1))
    from_chip = lax.ppermute(edge_chip, "space", swaps(size, 0))

    kron, waves = pl.pallas_call(
        functools.partial(twiddle, freqs),
        out_shape=[
            jax.ShapeDtypeStruct((freqs * 16, STEPS * 8), jnp.bfloat16),
            f32(2 * STEPS, LANES),
        ],
        in_specs=[whole()],
        out_specs=[whole()] * 2,
        cost_estimate=cost(100_000, 40_000),
        compiler_params=params(512),
        name="twiddle",
    )(block)

    row_spectra = pl.pallas_call(
        functools.partial(pack_spectra, freqs),
        out_shape=VMEM((members, PARTS * freqs, LANES), jnp.bfloat16),
        in_specs=[whole()],
        out_specs=whole(),
        cost_estimate=cost(2_000_000, 1_000_000),
        compiler_params=params(1536),
        name="pack_spectra",
    )(held)
    message = pl.pallas_call(
        pack_rows,
        out_shape=VMEM((members, message_rows, LANES), jnp.bfloat16),
        in_specs=[whole()] * 4,
        out_specs=whole(),
        scratch_shapes=[VMEM((MSG_ROWS, LANES), jnp.float32)],
        cost_estimate=cost(100_000, 300_000),
        compiler_params=params(2048),
        name="pack_rows",
    )(block, from_chip, from_link, row_spectra)
    received = lax.all_to_all(message, ("role", "freq"), 0, 0, tiled=True)

    fields_out, spectra_out, gradient = pl.pallas_call(
        functools.partial(finish, groups, freqs, count),
        out_shape=[
            f32(NFIELD, 2, LANES),
            f32(freqs * PARTS * rows_all, LANES),
            f32(1, LANES),
        ],
        in_specs=[whole()] * 5,
        out_specs=[whole(pl.ANY)] * 3,
        scratch_shapes=[
            VMEM((members * MSG_ROWS, LANES), jnp.float32),
            VMEM(((2 * NFIELD + 1) * rows_all, LANES), jnp.float32),
            VMEM((2 * rows_all, LANES), jnp.float32),
            VMEM((2, STEPS * rows_all, 2 * LANES), jnp.float32),
            VMEM((2 * STEPS, LANES), jnp.float32),
            VMEM((1, LANES), jnp.float32),
            VMEM((2 * STEPS * 2 * rows_all, LANES), jnp.float32),
            VMEM((2, NFIELD, rows_all, LANES), jnp.float32),
            VMEM((2, STEPS, 2 * LANES), jnp.float32),
            VMEM((NFIELD, 2, LANES), jnp.float32),
            VMEM((1, LANES), jnp.float32),
            VMEM((freqs * PARTS * rows_all, LANES), jnp.float32),
            pltpu.SemaphoreType.DMA((6,)),
        ],
        cost_estimate=cost(20_000_000, 2_000_000),
        compiler_params=params(4096),
        name="finish",
    )(received, kron, waves, held, shades)
    return fields_out[None], spectra_out.reshape(spectra.shape), gradient


def solution(mesh):
    return jax.shard_map(
        program,
        mesh=mesh,
        in_specs=(
            P("role", None, "freq", "space"),
            P("role", "freq", None, None, "space"),
            P("freq"),
            P("freq"),
            P("freq", "space"),
            P(),
            P("role", None),
            P("role", None, None),
        ),
        out_specs=(
            P("role", None, "freq", "space"),
            P("role", "freq", None, None, "space"),
            P(("role", "freq"), "space"),
        ),
        check_vma=False,
    )
```
